32 devices in a mesh: region: 2 (over x), orig: 2 (over core), shel: 8 (over z, y).
Axes of the slice: x: 2, y: 2, z: 4, core: 2. Of those that a mesh axis runs over, the one named last changes fastest.
Arguments:
- anchor_embed: float32 [32, 65536], P(None, ('region', 'orig')), parts along dimension 1, may hold values from -7 to 7
- shelter_embed: float32 [32, 2048], P(None, ('region', 'shel')), parts along dimension 1, may hold values from -7 to 7
- hazard: float32 [2, 2048], P(None, ('region', 'shel')), parts along dimension 1, may hold values from 0 to 1
- shelter_pot: float32 [2, 2048], P(None, ('region', 'shel')), parts along dimension 1, may hold values from -30 to 29
Outputs:
- anchor_pot: float32 [2, 65536], P(None, ('region', 'orig')), parts along dimension 1
- new_shelter_pot: float32 [2, 2048], P(None, ('region', 'shel')), parts along dimension 1
The draws below stay inside these ranges and needn't reach their ends.
There are 2 independent parts, one for each index of `region`. The reference program is written for one: setup_inputs(seed, part) draws one part's arguments, and reference() takes and returns one part's arrays. A program takes and returns all parts, laid end to end along the dimension named above; each array names one. Nothing has to cross between parts.
All inputs are finite; a program needn't handle non-finite values.
Results may differ from the reference program's by a relative error of at most 0.0003.
Values sent between devices are 32-bit elements; how exact they have to be, the bound alone decides.
No kernel may reach another device: no remote copies, remote signals or barrier semaphores. Data moves between devices by JAX's collectives and lax.ppermute only.
A program may use at most 64 MiB of HBM per device.

```python
import math
import jax
import jax.numpy as jnp
from jax import lax

EMB = 32
SCEN = 2
SHEL_DEV = 128
ANCHORS = 32768
SHELTERS = 1024


corner = 7.0


partner = 7.0 - 0.7071067811865476


def drawn(key):
    blocks = SHELTERS // SHEL_DEV
    half = SHEL_DEV // 2
    offset = jax.random.randint(jax.random.fold_in(key, 101), (blocks,), 0, half - 1)
    upper_half = jax.random.randint(jax.random.fold_in(key, 102), (blocks,), 0, 2)
    starts = jnp.arange(blocks, dtype=jnp.int32) * SHEL_DEV + offset
    warm = starts + upper_half * half
    chill = starts + (1 - upper_half) * half
    signs_warm = (2 * jax.random.randint(jax.random.fold_in(key, 103), (EMB, blocks), 0, 2) - 1).astype(jnp.float32)
    signs_chill = (2 * jax.random.randint(jax.random.fold_in(key, 104), (EMB, blocks), 0, 2) - 1).astype(jnp.float32)
    order = jax.random.permutation(jax.random.fold_in(key, 105), ANCHORS)[:4 * blocks]
    return (warm, chill, signs_warm, signs_chill, order)


def drawn_embed(key, columns):
    values = jnp.clip(jax.random.normal(key, (EMB, columns), jnp.float32), -6.0, 6.0)
    return values


def hazard_values(key):
    values = jax.random.uniform(jax.random.fold_in(key, 108), (SCEN, SHELTERS), jnp.float32, 0.0, 1.0)
    return values


def draw_anchor_embed(key, part):
    warm, chill, signs_warm, signs_chill, order = drawn(key)
    blocks = warm.shape[0]
    values = drawn_embed(jax.random.fold_in(key, 106), ANCHORS)
    values = values.at[:, order[0:blocks]].set(corner * signs_warm)
    values = values.at[:, order[blocks:2 * blocks]].set(partner * signs_warm)
    values = values.at[:, order[2 * blocks:3 * blocks]].set(corner * signs_chill)
    values = values.at[:, order[3 * blocks:4 * blocks]].set(partner * signs_chill)
    return values.astype(jnp.float32)


def draw_shelter_embed(key, part):
    warm, chill, signs_warm, signs_chill, order = drawn(key)
    values = drawn_embed(jax.random.fold_in(key, 107), SHELTERS)
    values = values.at[:, warm].set(corner * signs_warm)
    values = values.at[:, warm + 1].set(partner * signs_warm)
    values = values.at[:, chill].set(corner * signs_chill)
    values = values.at[:, chill + 1].set(partner * signs_chill)
    return values.astype(jnp.float32)


def draw_hazard(key, part):
    return hazard_values(key).astype(jnp.float32)


def draw_shelter_pot(key, part):
    warm, chill, signs_warm, signs_chill, order = drawn(key)
    hazard = hazard_values(key)
    sub = jax.random.fold_in(key, 109)
    values = jnp.clip(0.5 * jax.random.normal(sub, (SCEN, SHELTERS), jnp.float32), -2.0, 2.0)
    values = values.at[:, warm].set(28.0 + hazard[:, warm])
    values = values.at[:, warm + 1].set(28.0 + hazard[:, warm + 1])
    values = values.at[:, chill].set(-30.0 + hazard[:, chill])
    values = values.at[:, chill + 1].set(-30.0 + hazard[:, chill + 1])
    return values.astype(jnp.float32)


def setup_inputs(seed: int = 0, part: int = 0) -> dict:
    key_of = jax.random.split(jax.random.key(seed), 5)
    own_keys = jax.random.split(jax.random.fold_in(key_of[4], part), 5)
    return {
        "anchor_embed": draw_anchor_embed(jax.random.fold_in(jax.random.fold_in(key_of[4], part), 71), part),
        "shelter_embed": draw_shelter_embed(jax.random.fold_in(jax.random.fold_in(key_of[4], part), 71), part),
        "hazard": draw_hazard(jax.random.fold_in(jax.random.fold_in(key_of[4], part), 71), part),
        "shelter_pot": draw_shelter_pot(jax.random.fold_in(jax.random.fold_in(key_of[4], part), 71), part),
    }


EPSILON = 0.25


def tile_cost(xblock, shelter_embed, hazard):
    cross = jnp.dot(xblock.T, shelter_embed, precision=lax.Precision.HIGHEST, preferred_element_type=jnp.float32)
    xnorm = jnp.sum(xblock * xblock, axis=0)
    ynorm = jnp.sum(shelter_embed * shelter_embed, axis=0)
    dist = (xnorm[:, None] + ynorm[None, :] - 2.0 * cross) / xblock.shape[0]
    return dist[None, :, :] + hazard[:, None, :]


def reference(anchor_embed, shelter_embed, hazard, shelter_pot):
    anchors = anchor_embed.shape[1]
    shelters = shelter_embed.shape[1]
    block = math.gcd(anchors, 1024)
    count = anchors // block

    def row_block(index):
        xblock = lax.dynamic_slice_in_dim(anchor_embed, (index * block).astype(jnp.int32), block, 1)
        score = (shelter_pot[:, None, :] - tile_cost(xblock, shelter_embed, hazard)) / EPSILON
        top = jnp.max(score, axis=2)
        return top + jnp.log(jnp.sum(jnp.exp(score - top[:, :, None]), axis=2))

    pieces = lax.map(row_block, jnp.arange(count, dtype=jnp.int32))
    row_lse = jnp.transpose(pieces, (1, 0, 2)).reshape(hazard.shape[0], anchors)
    anchor_pot = -EPSILON * math.log(shelters) - EPSILON * row_lse

    def col_step(carry, index):
        top, total = carry
        start = (index * block).astype(jnp.int32)
        xblock = lax.dynamic_slice_in_dim(anchor_embed, start, block, 1)
        fblock = lax.dynamic_slice_in_dim(anchor_pot, start, block, 1)
        score = (fblock[:, :, None] - tile_cost(xblock, shelter_embed, hazard)) / EPSILON
        block_top = jnp.max(score, axis=1)
        newtop = jnp.maximum(top, block_top)
        total = total * jnp.exp(top - newtop) + jnp.sum(jnp.exp(score - newtop[:, None, :]), axis=1)
        return (newtop, total), None

    start_top = jnp.full(hazard.shape, -jnp.inf, dtype=jnp.float32)
    start_total = jnp.zeros(hazard.shape, dtype=jnp.float32)
    (top, total), unused = lax.scan(col_step, (start_top, start_total), jnp.arange(count, dtype=jnp.int32))
    new_shelter_pot = -EPSILON * math.log(anchors) - EPSILON * (top + jnp.log(total))
    return anchor_pot, new_shelter_pot
```

```python
import functools
import math

import jax
import jax.numpy as jnp
from jax import lax
from jax.experimental import pallas as pl
from jax.experimental.pallas import tpu as pltpu
from jax.sharding import PartitionSpec as P

EPSILON = 0.25
SCALE = math.log2(math.e) / EPSILON
SPREAD = 36.0
DEPTH = 256


def three(v):
    a = v.astype(jnp.bfloat16).astype(jnp.float32)
    rest = v - a
    b = rest.astype(jnp.bfloat16).astype(jnp.float32)
    return a, b, (rest - b).astype(jnp.bfloat16).astype(jnp.float32)


def rows_of(values, count):
    width = next(v.shape[1] for v in values if not isinstance(v, float))
    index = lax.broadcasted_iota(jnp.int32, (count, width), 0)
    out = jnp.zeros((count, width), jnp.float32)
    for k, v in enumerate(values):
        out = jnp.where(index == k, v, out)
    return out


def x_side(x):
    emb = x.shape[0]
    x0, x1, x2 = three(x)
    norm = jnp.sum(x * x, axis=0, keepdims=True) * (-SCALE / emb)
    misc = rows_of((*three(norm), 1.0, 1.0, 1.0), DEPTH - 6 * emb)
    return jnp.concatenate([x0, x0, x1, x1, x0, x2, misc], axis=0).astype(jnp.bfloat16)


def gap_of(z, emb):
    h0, h1, f0, f1 = (z[emb + k : emb + k + 1] for k in range(4))
    return SCALE * ((f1 - h1) - (f0 - h0))


def y_side(z, emb):
    y = z[:emb]
    y0, y1, y2 = three(y * (2.0 * SCALE / emb))
    bias = SCALE * (z[emb + 2 : emb + 3] - z[emb : emb + 1]) - jnp.sum(y * y, axis=0, keepdims=True) * (SCALE / emb)
    misc = rows_of((1.0, 1.0, 1.0, *three(bias)), DEPTH - 6 * emb)
    side = jnp.concatenate([y0, y1, y0, y1, y2, y0, misc], axis=0)
    return side.T.astype(jnp.bfloat16)


def across(row):
    return jnp.broadcast_to(row, (128, row.shape[1])).T


def wide(block, width):
    return jnp.concatenate([block] * (width // 128), axis=1)


def score(side, other):
    return lax.dot_general(side, other, (((1,), (0,)), ((), ())), preferred_element_type=jnp.float32)


def row_sums(side_ref, ratio_ref, start, stop, other, state):
    width = other.shape[1]
    columns = side_ref.shape[1]
    per = max(1, 256 // columns)

    def some(b, count, state):
        top, sum0, sum1 = state
        v = score(side_ref[pl.ds(b, count)].reshape(count * columns, DEPTH), other)
        r = wide(ratio_ref[pl.ds(b, count)].reshape(count * columns, 128), width)
        v = v.reshape(count * columns // 8, 8, width)
        new = jnp.max(v, axis=0)
        if top is not None:
            new = jnp.maximum(top, new)
        e = jnp.exp2(v - new)
        add0, add1 = jnp.sum(e, axis=0), jnp.sum(e * r.reshape(v.shape), axis=0)
        if top is None:
            return new, add0, add1
        less = jnp.exp2(top - new)
        return new, sum0 * less + add0, sum1 * less + add1

    count = min(per, stop - start)
    state = some(start, count, state)
    chunks = (stop - start) // count
    if chunks <= 4:
        for k in range(1, chunks):
            state = some(start + k * count, count, state)
        return state
    return lax.fori_loop(1, chunks, lambda k, s: some(start + k * count, count, s), state)


def one_row(state):
    top, sum0, sum1 = state
    high = jnp.max(top, axis=0, keepdims=True)
    less = jnp.exp2(top - high)
    return high, jnp.sum(sum0 * less, axis=0, keepdims=True), jnp.sum(sum1 * less, axis=0, keepdims=True)


def prepare(z_ref, emb, block, side_ref, ratio_ref, slot):
    z = z_ref[block]
    side_ref[slot] = y_side(z, emb)
    ratio_ref[slot] = across(jnp.exp2(jnp.clip(gap_of(z, emb), -SPREAD, SPREAD)))


def fetches(x_hbm, x_ref, sems, tile):
    def fetch(t):
        at = pl.ds(pl.multiple_of(t * tile, tile), tile)
        return pltpu.make_async_copy(x_hbm.at[:, at], x_ref.at[:, at], sems.at[t])

    def begin(t, carry):
        fetch(t).start()
        return carry

    lax.fori_loop(0, x_ref.shape[1] // tile, begin, 0)
    return fetch


def part_kernel(emb, tile, x_hbm, z_ref, stat_ref, x_ref, sems, side_ref, ratio_ref):
    blocks = z_ref.shape[0]
    fetch = fetches(x_hbm, x_ref, sems, tile)
    for b in range(blocks):
        prepare(z_ref, emb, b, side_ref, ratio_ref, b)

    def step(t, carry):
        fetch(t).wait()
        for part in range(0, tile, 256):
            at = pl.ds(pl.multiple_of(t * tile + part, 256), 256)
            state = row_sums(side_ref, ratio_ref, 0, blocks, x_side(x_ref[:, at]), (None, None, None))
            for k, v in enumerate(one_row(state)):
                stat_ref[k : k + 1, at] = v
        return carry

    lax.fori_loop(0, x_ref.shape[1] // tile, step, 0)


def last_kernel(emb, tile, shelters, known, x_hbm, z_ref, *refs):
    stats = refs[: len(known)]
    anchor_ref, column_ref, x_ref, sems, side_ref, ratio_ref, other_ref, lse_ref = refs[len(known) :]
    blocks, _, columns = z_ref.shape
    first = sum(known)
    left = blocks - first
    tiles = x_ref.shape[1] // tile
    f32 = jnp.float32
    fetch = fetches(x_hbm, x_ref, sems, tile)
    for b in range(left):
        prepare(z_ref, emb, first + b, side_ref, ratio_ref, b)
    prepare(z_ref, emb, 0, side_ref, ratio_ref, left)
    spread = lax.fori_loop(0, blocks, lambda b, w: jnp.maximum(w, jnp.max(jnp.abs(gap_of(z_ref[b], emb)))), f32(0.0))
    near = spread <= SPREAD

    def row_step(t, carry):
        fetch(t).wait()
        for part in range(0, tile, 256):
            at = pl.ds(pl.multiple_of(t * tile + part, 256), 256)
            other = x_side(x_ref[:, at])
            other_ref[:, at] = other
            states = [one_row(row_sums(side_ref, ratio_ref, 0, left, other, (None, None, None)))]
            states += [tuple(ref[k : k + 1, at] for k in range(3)) for ref in stats]
            high = functools.reduce(jnp.maximum, [s[0] for s in states])
            less = [jnp.exp2(s[0] - high) for s in states]
            for k in range(2):
                total = sum(s[1 + k] * m for s, m in zip(states, less))
                lse = high + jnp.log2(total)
                lse_ref[k : k + 1, at] = lse
                anchor_ref[k : k + 1, at] = (-EPSILON * math.log(shelters)) - (EPSILON * math.log(2.0)) * lse
        return carry

    lax.fori_loop(0, tiles, row_step, 0)

    def column_step(t, state):
        top, sum0, sum1 = state
        at = pl.ds(pl.multiple_of(t * tile, tile), tile)
        lse = lse_ref[0:1, at]
        weight = jnp.exp2(jnp.clip(lse - lse_ref[1:2, at], -SPREAD, SPREAD))
        v = score(side_ref[left], other_ref[:, at]) - lse
        parts = [slice(k * 128, (k + 1) * 128) for k in range(tile // 128)]
        new = functools.reduce(jnp.maximum, [v[:, p] for p in parts], top)
        less = jnp.exp2(top - new)
        sum0, sum1 = sum0 * less, sum1 * less
        for p in parts:
            e = jnp.exp2(v[:, p] - new)
            sum0 = sum0 + e
            sum1 = sum1 + e * weight[:, p]
        return new, sum0, sum1

    zero = jnp.zeros((columns, 128), f32)
    top, sum0, sum1 = lax.fori_loop(0, tiles, column_step, (jnp.full((columns, 128), -1e30, f32), zero, zero))
    z = z_ref[0]
    h0, h1, f0, f1 = (z[emb + k : emb + k + 1] for k in range(4))
    offset = (-SCALE * f0 - math.log2(shelters), -SCALE * (h1 + f0 - h0) - math.log2(shelters))
    top, sum0, sum1 = top.T, sum0.T, sum1.T
    high = jnp.max(top, axis=0, keepdims=True)
    less = jnp.exp2(top - high)
    column_ref[0:1, :] = high + jnp.log2(jnp.sum(sum0 * less, axis=0, keepdims=True)) + offset[0]
    column_ref[1:2, :] = high + jnp.log2(jnp.sum(sum1 * less, axis=0, keepdims=True)) + offset[1]

    @pl.when(jnp.logical_not(near))
    def _():
        own = side_ref[left]
        for s in range(2):

            def exact(t, carry):
                at = pl.ds(pl.multiple_of(t * tile, tile), tile)

                def block(b, state):
                    side_ref[0] = y_side(z_ref[b], emb)
                    v = score(side_ref[0], other_ref[:, at])
                    if s:
                        v = v + wide(across(gap_of(z_ref[b], emb)), tile)
                    new = jnp.maximum(state[0], jnp.max(v, axis=0, keepdims=True))
                    return new, state[1] * jnp.exp2(state[0] - new) + jnp.sum(jnp.exp2(v - new), axis=0, keepdims=True)

                high, total = lax.fori_loop(0, blocks, block, (jnp.full((1, tile), -1e30, f32), jnp.zeros((1, tile), f32)))
                lse = high + jnp.log2(total)
                lse_ref[s : s + 1, at] = lse
                anchor_ref[s : s + 1, at] = (-EPSILON * math.log(shelters)) - (EPSILON * math.log(2.0)) * lse
                return carry

            lax.fori_loop(0, tiles, exact, 0)

            def column(t, state):
                at = pl.ds(pl.multiple_of(t * tile, tile), tile)
                v = score(own, other_ref[:, at]) - lse_ref[s : s + 1, at]
                new, total = state
                for k in range(tile // 128):
                    new = jnp.maximum(new, v[:, k * 128 : (k + 1) * 128])
                total = total * jnp.exp2(state[0] - new)
                for k in range(tile // 128):
                    total = total + jnp.exp2(v[:, k * 128 : (k + 1) * 128] - new)
                return new, total

            high, total = lax.fori_loop(0, tiles, column, (jnp.full((columns, 128), -1e30, f32), zero))
            high, total = high.T, total.T
            most = jnp.max(high, axis=0, keepdims=True)
            total = jnp.sum(total * jnp.exp2(high - most), axis=0, keepdims=True)
            column_ref[s : s + 1, :] = most + jnp.log2(total) + offset[s]


def on_device(anchor_embed, shelter_embed, hazard, shelter_pot):
    emb, rows = anchor_embed.shape
    columns = shelter_embed.shape[1]
    anchors = rows * lax.axis_size("orig")
    groups = lax.axis_size("shel")
    shelters = columns * groups
    tile = math.gcd(rows, 1024)
    f32 = jnp.float32
    vmem = pl.BlockSpec(memory_space=pltpu.VMEM)
    hbm = pl.BlockSpec(memory_space=pl.ANY)

    def scratch(blocks):
        return [
            pltpu.VMEM((emb, rows), f32),
            pltpu.SemaphoreType.DMA((rows // tile,)),
            pltpu.VMEM((blocks, columns, DEPTH), jnp.bfloat16),
            pltpu.VMEM((blocks, columns, 128), f32),
        ]

    def cost(blocks):
        return pl.CostEstimate(flops=2 * rows * columns * blocks * DEPTH, bytes_accessed=4 * rows * emb, transcendentals=rows * columns * blocks)

    def part(some):
        return pl.pallas_call(
            functools.partial(part_kernel, emb, tile),
            out_shape=jax.ShapeDtypeStruct((8, rows), f32),
            in_specs=[hbm, vmem],
            out_specs=vmem,
            scratch_shapes=scratch(some.shape[0]),
            compiler_params=pltpu.CompilerParams(vmem_limit_bytes=32 * 2**20),
            cost_estimate=cost(some.shape[0]),
        )(anchor_embed, some)

    every = jnp.concatenate([shelter_embed, hazard, shelter_pot], axis=0)[None]
    stats, known = [], []
    if groups & (groups - 1) == 0:
        far = 1
        while far < groups:
            got = lax.ppermute(every, "shel", [(k, k ^ far) for k in range(groups)])
            if far == 2:
                stats.append(part(every))
                known.append(far)
            elif far > 2:
                stats.append(part(every[far // 2 :]))
                known.append(far // 2)
            every = jnp.concatenate([every, got], axis=0)
            far *= 2
    else:
        other = [lax.ppermute(every, "shel", [(k, (k + d) % groups) for k in range(groups)]) for d in range(1, groups)]
        every = jnp.concatenate([every, *other])
    left = groups - sum(known)

    anchor_pot, column = pl.pallas_call(
        functools.partial(last_kernel, emb, tile, shelters, tuple(known)),
        out_shape=(jax.ShapeDtypeStruct((2, rows), f32), jax.ShapeDtypeStruct((2, columns), f32)),
        in_specs=[hbm] + [vmem] * (1 + len(stats)),
        out_specs=(vmem, vmem),
        scratch_shapes=[*scratch(left + 1), pltpu.VMEM((DEPTH, rows), jnp.bfloat16), pltpu.VMEM((2, rows), f32)],
        compiler_params=pltpu.CompilerParams(vmem_limit_bytes=48 * 2**20),
        cost_estimate=cost(left + 1),
    )(anchor_embed, every, *stats)

    halves = lax.axis_size("orig")
    parts = [column]
    for d in range(1, halves):
        parts.append(lax.ppermute(column, "orig", [(k, (k + d) % halves) for k in range(halves)]))
    high = functools.reduce(jnp.maximum, parts)
    total = sum(jnp.exp2(part - high) for part in parts)
    new_shelter_pot = -EPSILON * math.log(anchors) - (EPSILON * math.log(2.0)) * (high + jnp.log2(total))
    return anchor_pot, new_shelter_pot


def solution(mesh):
    placed = (
        P(None, ("region", "orig")),
        P(None, ("region", "shel")),
        P(None, ("region", "shel")),
        P(None, ("region", "shel")),
    )
    return jax.shard_map(
        on_device,
        mesh=mesh,
        in_specs=placed,
        out_specs=(P(None, ("region", "orig")), P(None, ("region", "shel"))),
        check_vma=False,
    )
```

```python
import functools
import math

import jax
import jax.numpy as jnp
from jax import lax
from jax.experimental import pallas as pl
from jax.experimental.pallas import tpu as pltpu
from jax.sharding import PartitionSpec as P

EPSILON = 0.25
SCALE = math.log2(math.e) / EPSILON
SPREAD = 36.0
DEPTH = 256


def three(v):
    a = v.astype(jnp.bfloat16).astype(jnp.float32)
    rest = v - a
    b = rest.astype(jnp.bfloat16).astype(jnp.float32)
    return a, b, (rest - b).astype(jnp.bfloat16).astype(jnp.float32)


def rows_of(values, count):
    width = next(v.shape[1] for v in values if not isinstance(v, float))
    index = lax.broadcasted_iota(jnp.int32, (count, width), 0)
    out = jnp.zeros((count, width), jnp.float32)
    for k, v in enumerate(values):
        out = jnp.where(index == k, v, out)
    return out


def x_side(x):
    emb = x.shape[0]
    x0, x1, x2 = three(x)
    norm = jnp.sum(x * x, axis=0, keepdims=True) * (-SCALE / emb)
    misc = rows_of((*three(norm), 1.0, 1.0, 1.0), DEPTH - 6 * emb)
    return jnp.concatenate([x0, x0, x1, x1, x0, x2, misc], axis=0).astype(jnp.bfloat16)


def gap_of(z, emb):
    h0, h1, f0, f1 = (z[emb + k : emb + k + 1] for k in range(4))
    return SCALE * ((f1 - h1) - (f0 - h0))


def y_side(z, emb):
    y = z[:emb]
    y0, y1, y2 = three(y * (2.0 * SCALE / emb))
    bias = SCALE * (z[emb + 2 : emb + 3] - z[emb : emb + 1]) - jnp.sum(y * y, axis=0, keepdims=True) * (SCALE / emb)
    misc = rows_of((1.0, 1.0, 1.0, *three(bias)), DEPTH - 6 * emb)
    side = jnp.concatenate([y0, y1, y0, y1, y2, y0, misc], axis=0)
    return side.T.astype(jnp.bfloat16)


def across(row):
    return jnp.broadcast_to(row, (128, row.shape[1])).T


def wide(block, width):
    return jnp.concatenate([block] * (width // 128), axis=1)


def score(side, other):
    return lax.dot_general(side, other, (((1,), (0,)), ((), ())), preferred_element_type=jnp.float32)


def row_sums(side, ratio, other):
    width = other.shape[1]
    count = side.shape[0]
    chunk = math.gcd(count, 128)
    v = score(side, other)
    state = None
    for c in range(0, count, chunk):
        part = v[c : c + chunk].reshape(chunk // 8, 8, width)
        r = wide(ratio[c : c + chunk], width).reshape(part.shape)
        new = jnp.max(part, axis=0)
        if state is not None:
            new = jnp.maximum(state[0], new)
        e = jnp.exp2(part - new)
        add0, add1 = jnp.sum(e, axis=0), jnp.sum(e * r, axis=0)
        if state is not None:
            less = jnp.exp2(state[0] - new)
            add0, add1 = state[1] * less + add0, state[2] * less + add1
        state = new, add0, add1
    return state


def merged(first, second):
    if first is None:
        return second
    high = jnp.maximum(first[0], second[0])
    one, two = jnp.exp2(first[0] - high), jnp.exp2(second[0] - high)
    return (high, *(a * one + b * two for a, b in zip(first[1:], second[1:])))


def one_row(state):
    top, sum0, sum1 = state
    high = jnp.max(top, axis=0, keepdims=True)
    less = jnp.exp2(top - high)
    return high, jnp.sum(sum0 * less, axis=0, keepdims=True), jnp.sum(sum1 * less, axis=0, keepdims=True)


def prepare(z, emb, side_ref, ratio_ref, slot):
    columns = z.shape[1]
    at = pl.ds(slot * columns, columns)
    side_ref[at, :] = y_side(z, emb)
    ratio_ref[at, :] = across(jnp.exp2(jnp.clip(gap_of(z, emb), -SPREAD, SPREAD)))


def all_rows(side_ref, ratio_ref, other):
    count = side_ref.shape[0]
    if count <= 512:
        return row_sums(side_ref[...], ratio_ref[...], other)

    def step(k, state):
        at = pl.ds(pl.multiple_of(k * 512, 512), 512)
        return merged(state, row_sums(side_ref[at, :], ratio_ref[at, :], other))

    return lax.fori_loop(1, count // 512, step, row_sums(side_ref[:512], ratio_ref[:512], other))


def starting(pairs, half):
    return pl.multiple_of(lax.rem(lax.axis_index("shel"), pairs) * half, half)


def anchors_kernel(tile, x_hbm, other_ref, x_ref, sems):
    def fetch(t):
        at = pl.ds(pl.multiple_of(t * tile, tile), tile)
        return pltpu.make_async_copy(x_hbm.at[:, at], x_ref.at[:, at], sems.at[t])

    tiles = x_ref.shape[1] // tile

    def begin(t, carry):
        fetch(t).start()
        return carry

    def step(t, carry):
        fetch(t).wait()
        at = pl.ds(pl.multiple_of(t * tile, tile), tile)
        other_ref[:, at] = x_side(x_ref[:, at])
        return carry

    lax.fori_loop(0, tiles, begin, 0)
    lax.fori_loop(0, tiles, step, 0)


def part_kernel(emb, tile, pairs, other_ref, z_ref, stat_ref, side_ref, ratio_ref):
    half = stat_ref.shape[1]
    start = starting(pairs, half)
    for b in range(z_ref.shape[0]):
        prepare(z_ref[b], emb, side_ref, ratio_ref, b)

    def step(t, carry):
        for part in range(0, tile, 256):
            at = pl.multiple_of(t * tile + part, 256)
            other = other_ref[:, pl.ds(pl.multiple_of(start + at, 256), 256)]
            for k, v in enumerate(one_row(all_rows(side_ref, ratio_ref, other))):
                stat_ref[k : k + 1, pl.ds(at, 256)] = v
        return carry

    lax.fori_loop(0, half // tile, step, 0)


def spread_of(z_ref, emb):
    z = z_ref[...]
    h0, h1, f0, f1 = (z[:, emb + k, :] for k in range(4))
    return jnp.max(jnp.abs(SCALE * ((f1 - h1) - (f0 - h0))))


def rest_kernel(emb, tile, pairs, first, other_ref, z_ref, *refs):
    *stats, lse_ref, side_ref, ratio_ref = refs
    blocks, _, columns = z_ref.shape
    half = lse_ref.shape[1]
    start = starting(pairs, half)
    for b in range(first, blocks) if blocks <= 8 else ():
        prepare(z_ref[b], emb, side_ref, ratio_ref, b - first)
    if blocks > 8:

        def ready(b, carry):
            prepare(z_ref[b], emb, side_ref, ratio_ref, b - first)
            return carry

        lax.fori_loop(first, blocks, ready, 0)
    near = spread_of(z_ref, emb) <= SPREAD

    def step(t, carry):
        for part in range(0, tile, 256):
            at = pl.multiple_of(t * tile + part, 256)
            other = other_ref[:, pl.ds(pl.multiple_of(start + at, 256), 256)]
            at = pl.ds(at, 256)
            state = one_row(all_rows(side_ref, ratio_ref, other))
            for ref in stats:
                state = merged(state, tuple(ref[k : k + 1, at] for k in range(3)))
            for s in range(2):
                lse_ref[s : s + 1, at] = state[0] + jnp.log2(state[1 + s])
        return carry

    lax.fori_loop(0, half // tile, step, 0)

    @pl.when(jnp.logical_not(near))
    def _():
        own = pl.ds(0, columns)
        for s in range(2):

            def exact(t, carry):
                at = pl.multiple_of(t * 256, 256)
                other = other_ref[:, pl.ds(pl.multiple_of(start + at, 256), 256)]

                def block(b, state):
                    side_ref[own, :] = y_side(z_ref[b], emb)
                    v = score(side_ref[own, :], other)
                    if s:
                        v = v + wide(across(gap_of(z_ref[b], emb)), 256)
                    high = jnp.max(v, axis=0, keepdims=True)
                    return merged(state, (high, jnp.sum(jnp.exp2(v - high), axis=0, keepdims=True)))

                none = (jnp.full((1, 256), -1e30, jnp.float32), jnp.zeros((1, 256), jnp.float32))
                high, total = lax.fori_loop(0, blocks, block, none)
                lse_ref[s : s + 1, pl.ds(at, 256)] = high + jnp.log2(total)
                return carry

            lax.fori_loop(0, half // 256, exact, 0)


def column_sums(side, other_ref, start, lse_ref, tile, state_refs):
    columns = side.shape[0]

    def step(t, carry):
        at = pl.multiple_of(t * tile, tile)
        lse = lse_ref[0:1, pl.ds(at, tile)]
        weight = jnp.exp2(jnp.clip(lse - lse_ref[1:2, pl.ds(at, tile)], -SPREAD, SPREAD))
        lse, weight = jnp.broadcast_to(lse, (8, tile)), jnp.broadcast_to(weight, (8, tile))
        v = score(side, other_ref[:, pl.ds(pl.multiple_of(start + at, tile), tile)])
        parts = [slice(k, k + 128) for k in range(0, tile, 128)]
        for g in range(0, columns, 8):
            rows = slice(g, g + 8)
            u = [v[rows, p] - lse[:, p] for p in parts]
            top, sum0, sum1 = (ref[rows, :] for ref in state_refs)
            new = functools.reduce(jnp.maximum, u, top)
            less = jnp.exp2(top - new)
            e = [jnp.exp2(w - new) for w in u]
            state_refs[0][rows, :] = new
            state_refs[1][rows, :] = functools.reduce(jnp.add, e, sum0 * less)
            state_refs[2][rows, :] = functools.reduce(jnp.add, [w * weight[:, p] for w, p in zip(e, parts)], sum1 * less)
        return carry

    lax.fori_loop(0, lse_ref.shape[1] // tile, step, 0)


def columns_kernel(emb, tile, pairs, other_ref, z_ref, lse_ref, top_ref, sum0_ref, sum1_ref, side_ref):
    half = lse_ref.shape[1]
    side_ref[...] = y_side(z_ref[0], emb)
    top_ref[...] = jnp.full(top_ref.shape, -1e30, jnp.float32)
    sum0_ref[...] = jnp.zeros(sum0_ref.shape, jnp.float32)
    sum1_ref[...] = jnp.zeros(sum1_ref.shape, jnp.float32)
    column_sums(side_ref[...], other_ref, starting(pairs, half), lse_ref, tile, (top_ref, sum0_ref, sum1_ref))


def finish_kernel(emb, tile, pairs, shelters, other_ref, z_ref, *refs):
    lse_refs, refs = refs[:pairs], refs[pairs:]
    *old, anchor_ref, column_ref, top_ref, sum0_ref, sum1_ref, side_ref = refs
    half = lse_refs[0].shape[1]
    mine = lax.rem(lax.axis_index("shel"), pairs)
    near = spread_of(z_ref, emb) <= SPREAD
    starts = [pl.multiple_of((mine ^ k) * half, half) for k in range(pairs)]
    side_ref[...] = y_side(z_ref[0], emb)
    states = (top_ref, sum0_ref, sum1_ref)
    for new, ref in zip(states, old):
        new[...] = ref[...]
    for start, lse_ref in list(zip(starts, lse_refs))[1:]:
        column_sums(side_ref[...], other_ref, start, lse_ref, tile, states)
    z = z_ref[0]
    h0, h1, f0, f1 = (z[emb + k : emb + k + 1] for k in range(4))
    offset = (-SCALE * f0 - math.log2(shelters), -SCALE * (h1 + f0 - h0) - math.log2(shelters))

    def one(top, *sums):
        top = top.T
        high = jnp.max(top, axis=0, keepdims=True)
        less = jnp.exp2(top - high)
        return [high + jnp.log2(jnp.sum(s.T * less, axis=0, keepdims=True)) for s in sums]

    for s, v in enumerate(one(*(ref[...] for ref in states))):
        column_ref[s : s + 1, :] = v + offset[s]
    for start, lse_ref in zip(starts, lse_refs):
        anchor_ref[:, pl.ds(start, half)] = (-EPSILON * math.log(shelters)) - (EPSILON * math.log(2.0)) * lse_ref[...]

    @pl.when(jnp.logical_not(near))
    def _():
        for s in range(2):
            top_ref[...] = jnp.full(top_ref.shape, -1e30, jnp.float32)
            sum0_ref[...] = jnp.zeros(sum0_ref.shape, jnp.float32)
            for start, lse_ref in zip(starts, lse_refs):

                def column(t, carry):
                    at = pl.multiple_of(t * 256, 256)
                    other = other_ref[:, pl.ds(pl.multiple_of(start + at, 256), 256)]
                    v = score(side_ref[...], other) - lse_ref[s : s + 1, pl.ds(at, 256)]
                    top = top_ref[...]
                    new = jnp.maximum(top, jnp.maximum(v[:, :128], v[:, 128:]))
                    sum0_ref[...] = sum0_ref[...] * jnp.exp2(top - new) + jnp.exp2(v[:, :128] - new) + jnp.exp2(v[:, 128:] - new)
                    top_ref[...] = new
                    return carry

                lax.fori_loop(0, half // 256, column, 0)
            column_ref[s : s + 1, :] = one(top_ref[...], sum0_ref[...])[0] + offset[s]


def swapped(value, far, groups):
    return lax.ppermute(value, "shel", [(k, k ^ far) for k in range(groups)])


def on_device(anchor_embed, shelter_embed, hazard, shelter_pot):
    emb, rows = anchor_embed.shape
    columns = shelter_embed.shape[1]
    anchors = rows * lax.axis_size("orig")
    groups = lax.axis_size("shel")
    shelters = columns * groups
    pairs = 2 if groups % 2 == 0 else 1
    half = rows // pairs
    f32, bf16 = jnp.float32, jnp.bfloat16
    vmem = pl.BlockSpec(memory_space=pltpu.VMEM)

    def call(kernel, outs, ins, scratch, work, first=vmem):
        return pl.pallas_call(
            kernel,
            out_shape=outs,
            in_specs=[first] + [vmem] * (len(ins) - 1),
            out_specs=jax.tree.map(lambda _: vmem, outs),
            scratch_shapes=scratch,
            compiler_params=pltpu.CompilerParams(vmem_limit_bytes=24 * 2**20),
            cost_estimate=pl.CostEstimate(flops=2 * DEPTH * work, bytes_accessed=DEPTH * rows, transcendentals=work),
        )(*ins)

    def sides(blocks):
        return [pltpu.VMEM((blocks * columns, DEPTH), bf16), pltpu.VMEM((blocks * columns, 128), f32)]

    shape = jax.ShapeDtypeStruct
    every = jnp.concatenate([shelter_embed, hazard, shelter_pot], axis=0)[None]
    tile = math.gcd(rows, 1024)
    other = call(
        functools.partial(anchors_kernel, tile),
        shape((DEPTH, rows), bf16),
        [anchor_embed],
        [pltpu.VMEM((emb, rows), f32), pltpu.SemaphoreType.DMA((rows // tile,))],
        64 * rows,
        pl.BlockSpec(memory_space=pltpu.HBM),
    )

    tile = math.gcd(half, 1024)

    def part(some):
        blocks = some.shape[0]
        return call(
            functools.partial(part_kernel, emb, tile, pairs),
            shape((8, half), f32),
            [other, some],
            sides(blocks),
            half * columns * blocks,
        )

    stats, done = [], 0
    if groups & (groups - 1) == 0:
        far = 1
        while far < groups:
            got = swapped(every, far, groups)
            if far > 1:
                stats.append(part(every[done:]))
                done = far
            every = jnp.concatenate([every, got], axis=0)
            far *= 2
    else:
        blocks = [lax.ppermute(every, "shel", [(k, (k + d) % groups) for k in range(groups)]) for d in range(1, groups)]
        every = jnp.concatenate([every, *blocks])
    lse = call(
        functools.partial(rest_kernel, emb, tile, pairs, done),
        shape((2, half), f32),
        [other, every, *stats],
        sides(groups - done),
        half * columns * (groups - done),
    )

    tile = math.gcd(half, 2048)
    state = [shape((columns, 128), f32)] * 3
    lses = [lse] + ([swapped(lse, 1, groups)] if pairs == 2 else [])
    sums = call(
        functools.partial(columns_kernel, emb, tile, pairs),
        state,
        [other, every, lse],
        [pltpu.VMEM((columns, DEPTH), bf16)],
        half * columns,
    )
    anchor_pot, column = call(
        functools.partial(finish_kernel, emb, tile, pairs, shelters),
        (shape((2, rows), f32), shape((2, columns), f32)),
        [other, every, *lses, *sums],
        [pltpu.VMEM(s.shape, f32) for s in state] + [pltpu.VMEM((columns, DEPTH), bf16)],
        half * columns,
    )

    halves = lax.axis_size("orig")
    parts = [column]
    for d in range(1, halves):
        parts.append(lax.ppermute(column, "orig", [(k, (k + d) % halves) for k in range(halves)]))
    high = functools.reduce(jnp.maximum, parts)
    total = sum(jnp.exp2(part - high) for part in parts)
    new_shelter_pot = -EPSILON * math.log(anchors) - (EPSILON * math.log(2.0)) * (high + jnp.log2(total))
    return anchor_pot, new_shelter_pot


def solution(mesh):
    placed = (
        P(None, ("region", "orig")),
        P(None, ("region", "shel")),
        P(None, ("region", "shel")),
        P(None, ("region", "shel")),
    )
    return jax.shard_map(
        on_device,
        mesh=mesh,
        in_specs=placed,
        out_specs=(P(None, ("region", "orig")), P(None, ("region", "shel"))),
        check_vma=False,
    )
```

```python
import functools
import math

import jax
import jax.numpy as jnp
from jax import lax
from jax.experimental import pallas as pl
from jax.experimental.pallas import tpu as pltpu
from jax.sharding import PartitionSpec as P

EPSILON = 0.25
SCALE = math.log2(math.e) / EPSILON
SPREAD = 36.0
PIECE = 512
DEPTH = 256


def three(v):
    a = v.astype(jnp.bfloat16).astype(jnp.float32)
    rest = v - a
    b = rest.astype(jnp.bfloat16).astype(jnp.float32)
    return a, b, (rest - b).astype(jnp.bfloat16).astype(jnp.float32)


def rows_of(values, count):
    width = next(v.shape[1] for v in values if not isinstance(v, float))
    index = lax.broadcasted_iota(jnp.int32, (count, width), 0)
    out = jnp.zeros((count, width), jnp.float32)
    for k, v in enumerate(values):
        out = jnp.where(index == k, v, out)
    return out


def x_side(x):
    emb = x.shape[0]
    x0, x1, x2 = three(x)
    norm = jnp.sum(x * x, axis=0, keepdims=True) * (-SCALE / emb)
    misc = rows_of((*three(norm), 1.0, 1.0, 1.0), DEPTH - 6 * emb)
    return jnp.concatenate([x0, x0, x1, x1, x0, x2, misc], axis=0).astype(jnp.bfloat16)


def gap_of(z, emb):
    h0, h1, f0, f1 = (z[emb + k : emb + k + 1] for k in range(4))
    return SCALE * ((f1 - h1) - (f0 - h0))


def y_side(z, emb):
    y = z[:emb]
    y0, y1, y2 = three(y * (2.0 * SCALE / emb))
    bias = SCALE * (z[emb + 2 : emb + 3] - z[emb : emb + 1]) - jnp.sum(y * y, axis=0, keepdims=True) * (SCALE / emb)
    misc = rows_of((1.0, 1.0, 1.0, *three(bias)), DEPTH - 6 * emb)
    side = jnp.concatenate([y0, y1, y0, y1, y2, y0, misc], axis=0)
    return side.T.astype(jnp.bfloat16)


def across(row):
    return jnp.broadcast_to(row, (128, row.shape[1])).T


def wide(block, width):
    return jnp.concatenate([block] * (width // 128), axis=1)


def score(side, other):
    return lax.dot_general(side, other, (((1,), (0,)), ((), ())), preferred_element_type=jnp.float32)


def row_sums(side, ratio, other):
    width = other.shape[1]
    count = side.shape[0]
    chunk = math.gcd(count, 128)
    v = score(side, other)
    state = None
    for c in range(0, count, chunk):
        part = v[c : c + chunk].reshape(chunk // 8, 8, width)
        r = wide(ratio[c : c + chunk], width).reshape(part.shape)
        new = jnp.max(part, axis=0)
        if state is not None:
            new = jnp.maximum(state[0], new)
        e = jnp.exp2(part - new)
        add0, add1 = jnp.sum(e, axis=0), jnp.sum(e * r, axis=0)
        if state is not None:
            less = jnp.exp2(state[0] - new)
            add0, add1 = state[1] * less + add0, state[2] * less + add1
        state = new, add0, add1
    return state


def merged(first, second):
    if first is None:
        return second
    high = jnp.maximum(first[0], second[0])
    one, two = jnp.exp2(first[0] - high), jnp.exp2(second[0] - high)
    return (high, *(a * one + b * two for a, b in zip(first[1:], second[1:])))


def one_row(state):
    top, sum0, sum1 = state
    high = jnp.max(top, axis=0, keepdims=True)
    less = jnp.exp2(top - high)
    return high, jnp.sum(sum0 * less, axis=0, keepdims=True), jnp.sum(sum1 * less, axis=0, keepdims=True)


def prepare(z, emb, side_ref, ratio_ref, slot):
    columns = z.shape[1]
    at = pl.ds(slot * columns, columns)
    side_ref[at, :] = y_side(z, emb)
    ratio_ref[at, :] = across(jnp.exp2(jnp.clip(gap_of(z, emb), -SPREAD, SPREAD)))


def all_rows(side_ref, ratio_ref, other):
    count = side_ref.shape[0]
    if count <= 512:
        return row_sums(side_ref[...], ratio_ref[...], other)

    def step(k, state):
        at = pl.ds(pl.multiple_of(k * 512, 512), 512)
        return merged(state, row_sums(side_ref[at, :], ratio_ref[at, :], other))

    return lax.fori_loop(1, count // 512, step, row_sums(side_ref[:512], ratio_ref[:512], other))


def anchors_at(other_ref, start, width):
    first = start // 128
    return jnp.concatenate([other_ref[first + k] for k in range(width // 128)], axis=1)


def starting(pairs, half):
    return pl.multiple_of(lax.rem(lax.axis_index("shel"), pairs) * half, half)


def anchors_kernel(tile, x_ref, other_ref):
    def step(t, carry):
        side = x_side(x_ref[:, pl.ds(pl.multiple_of(t * tile, tile), tile)])
        for k in range(tile // 128):
            other_ref[t * (tile // 128) + k] = side[:, k * 128 : (k + 1) * 128]
        return carry

    lax.fori_loop(0, x_ref.shape[1] // tile, step, 0)


def part_kernel(emb, tile, pairs, other_ref, z_ref, stat_ref, side_ref, ratio_ref):
    half = stat_ref.shape[1]
    start = starting(pairs, half)
    for b in range(z_ref.shape[0]):
        prepare(z_ref[b], emb, side_ref, ratio_ref, b)

    def step(t, carry):
        found = []
        for part in range(0, tile, 256):
            at = pl.multiple_of(t * tile + part, 256)
            other = anchors_at(other_ref, start + at, 256)
            found.append((at, one_row(all_rows(side_ref, ratio_ref, other))))
        for at, state in found:
            for k, v in enumerate(state):
                stat_ref[k : k + 1, pl.ds(at, 256)] = v
        return carry

    lax.fori_loop(0, half // tile, step, 0)


def spread_of(z_ref, emb):
    z = z_ref[...]
    h0, h1, f0, f1 = (z[:, emb + k, :] for k in range(4))
    return jnp.max(jnp.abs(SCALE * ((f1 - h1) - (f0 - h0))))


def rest_kernel(emb, tile, pairs, first, other_ref, z_ref, *refs):
    *stats, lse_ref, side_ref, ratio_ref = refs
    blocks, _, columns = z_ref.shape
    half = lse_ref.shape[1]
    start = starting(pairs, half)
    for b in range(first, blocks) if blocks <= 8 else ():
        prepare(z_ref[b], emb, side_ref, ratio_ref, b - first)
    if blocks > 8:

        def ready(b, carry):
            prepare(z_ref[b], emb, side_ref, ratio_ref, b - first)
            return carry

        lax.fori_loop(first, blocks, ready, 0)
    near = spread_of(z_ref, emb) <= SPREAD

    def step(t, carry):
        found = []
        for part in range(0, tile, 256):
            at = pl.multiple_of(t * tile + part, 256)
            other = anchors_at(other_ref, start + at, 256)
            at = pl.ds(at, 256)
            state = one_row(all_rows(side_ref, ratio_ref, other))
            for ref in stats:
                state = merged(state, tuple(ref[k : k + 1, at] for k in range(3)))
            found.append((at, state))
        for at, state in found:
            for s in range(2):
                lse_ref[s : s + 1, at] = state[0] + jnp.log2(state[1 + s])
        return carry

    lax.fori_loop(0, half // tile, step, 0)

    @pl.when(jnp.logical_not(near))
    def _():
        own = pl.ds(0, columns)
        for s in range(2):

            def exact(t, carry):
                at = pl.multiple_of(t * 256, 256)
                other = anchors_at(other_ref, start + at, 256)

                def block(b, state):
                    side_ref[own, :] = y_side(z_ref[b], emb)
                    v = score(side_ref[own, :], other)
                    if s:
                        v = v + wide(across(gap_of(z_ref[b], emb)), 256)
                    high = jnp.max(v, axis=0, keepdims=True)
                    return merged(state, (high, jnp.sum(jnp.exp2(v - high), axis=0, keepdims=True)))

                none = (jnp.full((1, 256), -1e30, jnp.float32), jnp.zeros((1, 256), jnp.float32))
                high, total = lax.fori_loop(0, blocks, block, none)
                lse_ref[s : s + 1, pl.ds(at, 256)] = high + jnp.log2(total)
                return carry

            lax.fori_loop(0, half // 256, exact, 0)


def column_sums(side, other_ref, start, lse_ref, tile, state_refs):
    columns = side.shape[0]
    piece = math.gcd(tile, PIECE)

    def some(at, v):
        lse = lse_ref[0:1, pl.ds(at, piece)]
        weight = jnp.exp2(jnp.clip(lse - lse_ref[1:2, pl.ds(at, piece)], -SPREAD, SPREAD))
        lse, weight = jnp.broadcast_to(lse, (8, piece)), jnp.broadcast_to(weight, (8, piece))
        parts = [slice(k, k + 128) for k in range(0, piece, 128)]
        for g in range(0, columns, 8):
            rows = slice(g, g + 8)
            u = [v[rows, p] - lse[:, p] for p in parts]
            top, sum0, sum1 = (ref[rows, :] for ref in state_refs)
            new = functools.reduce(jnp.maximum, u, top)
            less = jnp.exp2(top - new)
            e = [jnp.exp2(w - new) for w in u]
            state_refs[0][rows, :] = new
            state_refs[1][rows, :] = functools.reduce(jnp.add, e, sum0 * less)
            state_refs[2][rows, :] = functools.reduce(jnp.add, [w * weight[:, p] for w, p in zip(e, parts)], sum1 * less)

    def step(t, carry):
        ats = [pl.multiple_of(t * tile + k, piece) for k in range(0, tile, piece)]
        scores = [score(side, anchors_at(other_ref, start + at, piece)) for at in ats]
        for at, v in zip(ats, scores):
            some(at, v)
        return carry

    lax.fori_loop(0, lse_ref.shape[1] // tile, step, 0)


def columns_kernel(emb, tile, pairs, other_ref, z_ref, lse_ref, top_ref, sum0_ref, sum1_ref, side_ref):
    half = lse_ref.shape[1]
    side_ref[...] = y_side(z_ref[0], emb)
    top_ref[...] = jnp.full(top_ref.shape, -1e30, jnp.float32)
    sum0_ref[...] = jnp.zeros(sum0_ref.shape, jnp.float32)
    sum1_ref[...] = jnp.zeros(sum1_ref.shape, jnp.float32)
    column_sums(side_ref[...], other_ref, starting(pairs, half), lse_ref, tile, (top_ref, sum0_ref, sum1_ref))


def finish_kernel(emb, tile, pairs, shelters, other_ref, z_ref, *refs):
    lse_refs, refs = refs[:pairs], refs[pairs:]
    *old, anchor_ref, column_ref, top_ref, sum0_ref, sum1_ref, side_ref = refs
    half = lse_refs[0].shape[1]
    mine = lax.rem(lax.axis_index("shel"), pairs)
    near = spread_of(z_ref, emb) <= SPREAD
    starts = [pl.multiple_of((mine ^ k) * half, half) for k in range(pairs)]
    side_ref[...] = y_side(z_ref[0], emb)
    states = (top_ref, sum0_ref, sum1_ref)
    for new, ref in zip(states, old):
        new[...] = ref[...]
    for start, lse_ref in list(zip(starts, lse_refs))[1:]:
        column_sums(side_ref[...], other_ref, start, lse_ref, tile, states)
    z = z_ref[0]
    h0, h1, f0, f1 = (z[emb + k : emb + k + 1] for k in range(4))
    offset = (-SCALE * f0 - math.log2(shelters), -SCALE * (h1 + f0 - h0) - math.log2(shelters))

    def one(top, *sums):
        top = top.T
        high = jnp.max(top, axis=0, keepdims=True)
        less = jnp.exp2(top - high)
        return [high + jnp.log2(jnp.sum(s.T * less, axis=0, keepdims=True)) for s in sums]

    for s, v in enumerate(one(*(ref[...] for ref in states))):
        column_ref[s : s + 1, :] = v + offset[s]
    for start, lse_ref in zip(starts, lse_refs):
        anchor_ref[:, pl.ds(start, half)] = (-EPSILON * math.log(shelters)) - (EPSILON * math.log(2.0)) * lse_ref[...]

    @pl.when(jnp.logical_not(near))
    def _():
        for s in range(2):
            top_ref[...] = jnp.full(top_ref.shape, -1e30, jnp.float32)
            sum0_ref[...] = jnp.zeros(sum0_ref.shape, jnp.float32)
            for start, lse_ref in zip(starts, lse_refs):

                def column(t, carry):
                    at = pl.multiple_of(t * 256, 256)
                    other = anchors_at(other_ref, start + at, 256)
                    v = score(side_ref[...], other) - lse_ref[s : s + 1, pl.ds(at, 256)]
                    top = top_ref[...]
                    new = jnp.maximum(top, jnp.maximum(v[:, :128], v[:, 128:]))
                    sum0_ref[...] = sum0_ref[...] * jnp.exp2(top - new) + jnp.exp2(v[:, :128] - new) + jnp.exp2(v[:, 128:] - new)
                    top_ref[...] = new
                    return carry

                lax.fori_loop(0, half // 256, column, 0)
            column_ref[s : s + 1, :] = one(top_ref[...], sum0_ref[...])[0] + offset[s]


def swapped(value, far, groups):
    return lax.ppermute(value, "shel", [(k, k ^ far) for k in range(groups)])


def on_device(anchor_embed, shelter_embed, hazard, shelter_pot):
    emb, rows = anchor_embed.shape
    columns = shelter_embed.shape[1]
    anchors = rows * lax.axis_size("orig")
    groups = lax.axis_size("shel")
    shelters = columns * groups
    pairs = 2 if groups % 2 == 0 else 1
    half = rows // pairs
    f32, bf16 = jnp.float32, jnp.bfloat16
    vmem = pl.BlockSpec(memory_space=pltpu.VMEM)

    def call(kernel, outs, ins, scratch, work):
        return pl.pallas_call(
            kernel,
            out_shape=outs,
            in_specs=[vmem] * len(ins),
            out_specs=jax.tree.map(lambda _: vmem, outs),
            scratch_shapes=scratch,
            compiler_params=pltpu.CompilerParams(vmem_limit_bytes=24 * 2**20),
            cost_estimate=pl.CostEstimate(flops=2 * DEPTH * work, bytes_accessed=DEPTH * rows, transcendentals=work),
        )(*ins)

    def sides(blocks):
        return [pltpu.VMEM((blocks * columns, DEPTH), bf16), pltpu.VMEM((blocks * columns, 128), f32)]

    shape = jax.ShapeDtypeStruct
    every = jnp.concatenate([shelter_embed, hazard, shelter_pot], axis=0)[None]
    other = call(
        functools.partial(anchors_kernel, math.gcd(rows, 1024)),
        shape((rows // 128, DEPTH, 128), bf16),
        [anchor_embed],
        [],
        64 * rows,
    )

    tile = math.gcd(half, 4096)

    def part(some):
        blocks = some.shape[0]
        return call(
            functools.partial(part_kernel, emb, tile, pairs),
            shape((8, half), f32),
            [other, some],
            sides(blocks),
            half * columns * blocks,
        )

    stats, done = [], 0
    if groups & (groups - 1) == 0:
        far = 1
        while far < groups:
            got = swapped(every, far, groups)
            if far > 1:
                stats.append(part(every[done:]))
                done = far
            every = jnp.concatenate([every, got], axis=0)
            far *= 2
    else:
        blocks = [lax.ppermute(every, "shel", [(k, (k + d) % groups) for k in range(groups)]) for d in range(1, groups)]
        every = jnp.concatenate([every, *blocks])
    lse = call(
        functools.partial(rest_kernel, emb, tile, pairs, done),
        shape((2, half), f32),
        [other, every, *stats],
        sides(groups - done),
        half * columns * (groups - done),
    )

    tile = math.gcd(half, 4096)
    state = [shape((columns, 128), f32)] * 3
    lses = [lse] + ([swapped(lse, 1, groups)] if pairs == 2 else [])
    sums = call(
        functools.partial(columns_kernel, emb, tile, pairs),
        state,
        [other, every, lse],
        [pltpu.VMEM((columns, DEPTH), bf16)],
        half * columns,
    )
    anchor_pot, column = call(
        functools.partial(finish_kernel, emb, tile, pairs, shelters),
        (shape((2, rows), f32), shape((2, columns), f32)),
        [other, every, *lses, *sums],
        [pltpu.VMEM(s.shape, f32) for s in state] + [pltpu.VMEM((columns, DEPTH), bf16)],
        half * columns,
    )

    halves = lax.axis_size("orig")
    parts = [column]
    for d in range(1, halves):
        parts.append(lax.ppermute(column, "orig", [(k, (k + d) % halves) for k in range(halves)]))
    high = functools.reduce(jnp.maximum, parts)
    total = sum(jnp.exp2(part - high) for part in parts)
    new_shelter_pot = -EPSILON * math.log(anchors) - (EPSILON * math.log(2.0)) * (high + jnp.log2(total))
    return anchor_pot, new_shelter_pot


def solution(mesh):
    placed = (
        P(None, ("region", "orig")),
        P(None, ("region", "shel")),
        P(None, ("region", "shel")),
        P(None, ("region", "shel")),
    )
    return jax.shard_map(
        on_device,
        mesh=mesh,
        in_specs=placed,
        out_specs=(P(None, ("region", "orig")), P(None, ("region", "shel"))),
        check_vma=False,
    )
```

```python
import functools
import math

import jax
import jax.numpy as jnp
from jax import lax
from jax.experimental import pallas as pl
from jax.experimental.pallas import tpu as pltpu
from jax.sharding import PartitionSpec as P

EPSILON = 0.25
SCALE = math.log2(math.e) / EPSILON
HUGE = 2.0**126
SPREAD = 36.0
PIECE = 512
DEPTH = 256


def three(v):
    a = v.astype(jnp.bfloat16).astype(jnp.float32)
    rest = v - a
    b = rest.astype(jnp.bfloat16).astype(jnp.float32)
    return a, b, (rest - b).astype(jnp.bfloat16).astype(jnp.float32)


def rows_of(values, count):
    width = next(v.shape[1] for v in values if not isinstance(v, float))
    index = lax.broadcasted_iota(jnp.int32, (count, width), 0)
    out = jnp.zeros((count, width), jnp.float32)
    for k, v in enumerate(values):
        out = jnp.where(index == k, v, out)
    return out


def x_side(x):
    emb = x.shape[0]
    x0, x1, x2 = three(x)
    norm = jnp.sum(x * x, axis=0, keepdims=True) * (-SCALE / emb)
    misc = rows_of((*three(norm), 1.0, 1.0, 1.0), DEPTH - 6 * emb)
    return jnp.concatenate([x0, x0, x1, x1, x0, x2, misc], axis=0).astype(jnp.bfloat16)


def gap_of(z, emb):
    h0, h1, f0, f1 = (z[emb + k : emb + k + 1] for k in range(4))
    return SCALE * ((f1 - h1) - (f0 - h0))


def y_side(z, emb):
    y = z[:emb]
    y0, y1, y2 = three(y * (2.0 * SCALE / emb))
    bias = SCALE * (z[emb + 2 : emb + 3] - z[emb : emb + 1]) - jnp.sum(y * y, axis=0, keepdims=True) * (SCALE / emb)
    misc = rows_of((1.0, 1.0, 1.0, *three(bias)), DEPTH - 6 * emb)
    side = jnp.concatenate([y0, y1, y0, y1, y2, y0, misc], axis=0)
    return side.T.astype(jnp.bfloat16)


def across(row):
    return jnp.broadcast_to(row, (128, row.shape[1])).T


def wide(block, width):
    return jnp.concatenate([block] * (width // 128), axis=1)


def score(side, other):
    return lax.dot_general(side, other, (((1,), (0,)), ((), ())), preferred_element_type=jnp.float32)


def row_sums(side, ratio, other):
    width = other.shape[1]
    count = side.shape[0]
    chunk = math.gcd(count, 128)
    v = score(side, other)
    state = None
    for c in range(0, count, chunk):
        part = v[c : c + chunk].reshape(chunk // 8, 8, width)
        r = wide(ratio[c : c + chunk], width).reshape(part.shape)
        new = jnp.max(part, axis=0)
        if state is not None:
            new = jnp.maximum(state[0], new)
        e = jnp.exp2(part - new)
        add0, add1 = jnp.sum(e, axis=0), jnp.sum(e * r, axis=0)
        if state is not None:
            less = jnp.exp2(state[0] - new)
            add0, add1 = state[1] * less + add0, state[2] * less + add1
        state = new, add0, add1
    return state


def merged(first, second):
    if first is None:
        return second
    high = jnp.maximum(first[0], second[0])
    one, two = jnp.exp2(first[0] - high), jnp.exp2(second[0] - high)
    return (high, *(a * one + b * two for a, b in zip(first[1:], second[1:])))


def one_row(state):
    top, sum0, sum1 = state
    high = jnp.max(top, axis=0, keepdims=True)
    less = jnp.exp2(top - high)
    return high, jnp.sum(sum0 * less, axis=0, keepdims=True), jnp.sum(sum1 * less, axis=0, keepdims=True)


def prepare(z, emb, side_ref, ratio_ref, slot):
    columns = z.shape[1]
    at = pl.ds(slot * columns, columns)
    side_ref[at, :] = y_side(z, emb)
    ratio_ref[at, :] = across(jnp.exp2(jnp.clip(gap_of(z, emb), -SPREAD, SPREAD)))


def all_rows(side_ref, ratio_ref, other):
    count = side_ref.shape[0]
    if count <= 512:
        return row_sums(side_ref[...], ratio_ref[...], other)

    def step(k, state):
        at = pl.ds(pl.multiple_of(k * 512, 512), 512)
        return merged(state, row_sums(side_ref[at, :], ratio_ref[at, :], other))

    return lax.fori_loop(1, count // 512, step, row_sums(side_ref[:512], ratio_ref[:512], other))


def anchors_at(other_ref, start, width):
    first = start // 128
    return jnp.concatenate([other_ref[first + k] for k in range(width // 128)], axis=1)


def starting(pairs, half):
    return pl.multiple_of(lax.rem(lax.axis_index("shel"), pairs) * half, half)


def anchors_kernel(tile, x_ref, other_ref):
    def step(t, carry):
        side = x_side(x_ref[:, pl.ds(pl.multiple_of(t * tile, tile), tile)])
        for k in range(tile // 128):
            other_ref[t * (tile // 128) + k] = side[:, k * 128 : (k + 1) * 128]
        return carry

    lax.fori_loop(0, x_ref.shape[1] // tile, step, 0)


def part_kernel(emb, tile, pairs, other_ref, z_ref, stat_ref, side_ref, ratio_ref):
    half = stat_ref.shape[1]
    start = starting(pairs, half)
    for b in range(z_ref.shape[0]):
        prepare(z_ref[b], emb, side_ref, ratio_ref, b)

    def step(t, carry):
        found = []
        for part in range(0, tile, 256):
            at = pl.multiple_of(t * tile + part, 256)
            other = anchors_at(other_ref, start + at, 256)
            found.append((at, one_row(all_rows(side_ref, ratio_ref, other))))
        for at, state in found:
            for k, v in enumerate(state):
                stat_ref[k : k + 1, pl.ds(at, 256)] = v
        return carry

    lax.fori_loop(0, half // tile, step, 0)


def spread_of(z_ref, emb):
    z = z_ref[...]
    h0, h1, f0, f1 = (z[:, emb + k, :] for k in range(4))
    return jnp.max(jnp.abs(SCALE * ((f1 - h1) - (f0 - h0))))


def hottest(z, side, emb):
    columns = z.shape[1]
    value = jnp.broadcast_to(z[emb + 2 : emb + 3] - z[emb : emb + 1], (8, columns))
    row = lax.broadcasted_iota(jnp.int32, (8, columns), 0)
    lane = lax.broadcasted_iota(jnp.int32, (8, columns), 1)
    value = jnp.where(lax.rem(lane, 8) == row, value, -1e30)
    pick = (value == jnp.max(value, axis=1, keepdims=True)).astype(jnp.float32)
    pick = pick / jnp.sum(pick, axis=1, keepdims=True)
    return score(pick.astype(jnp.bfloat16), side).astype(jnp.bfloat16)


def rest_kernel(emb, tile, pairs, first, other_ref, z_ref, *refs):
    *stats, lse_ref, side_ref, ratio_ref, hot_ref = refs
    blocks, _, columns = z_ref.shape
    half = lse_ref.shape[1]
    start = starting(pairs, half)
    count = side_ref.shape[0]
    lead = hot_ref.shape[0] - min(count, 512)
    f32 = jnp.float32

    def ready(b):
        prepare(z_ref[b], emb, side_ref, ratio_ref, b - first)
        side = side_ref[pl.ds((b - first) * columns, columns), :]
        hot_ref[pl.ds((b - first) * 8, 8), :] = hottest(z_ref[b], side, emb)

    if blocks <= 8:
        for b in range(first, blocks):
            ready(b)
    else:
        lax.fori_loop(first, blocks, lambda b, c: (ready(b), c)[1], 0)
    hot_ref[lead:, :] = side_ref[: hot_ref.shape[0] - lead, :]
    near = spread_of(z_ref, emb) <= SPREAD

    def known(at):
        state = None
        for ref in stats:
            state = merged(state, tuple(ref[k : k + 1, at] for k in range(3)))
        return state

    def store(found):
        for at, high, *totals in found:
            for s in range(2):
                lse_ref[s : s + 1, at] = high + jnp.log2(totals[s])

    def sums(v, shift, ratio):
        e = jnp.exp2(v - shift)
        w = e * wide(ratio, 256)
        return [jnp.sum(u.reshape(u.shape[0] // 8, 8, 256), axis=0) for u in (e, w)]

    def step(t, most):
        found = []
        for part in range(0, tile, 256):
            at = pl.multiple_of(t * tile + part, 256)
            other = anchors_at(other_ref, start + at, 256)
            at = pl.ds(at, 256)
            state = known(at)
            v = score(hot_ref[...], other)
            shift = jnp.max(v[:lead], axis=0, keepdims=True)
            if state is not None:
                shift = jnp.maximum(shift, state[0])
            totals = sums(v[lead:], shift, ratio_ref[: count if count < 512 else 512, :])
            if count > 512:

                def more(k, totals):
                    at = pl.ds(pl.multiple_of(k * 512, 512), 512)
                    add = sums(score(side_ref[at, :], other), shift, ratio_ref[at, :])
                    return [a + b for a, b in zip(totals, add)]

                totals = lax.fori_loop(1, count // 512, more, totals)
            totals = [jnp.sum(u, axis=0, keepdims=True) for u in totals]
            if state is not None:
                less = jnp.exp2(state[0] - shift)
                totals = [u + w * less for u, w in zip(totals, state[1:])]
            most = jnp.maximum(most, jnp.maximum(*totals))
            found.append((at, shift, *totals))
        store(found)
        return most

    most = lax.fori_loop(0, half // tile, step, jnp.zeros((1, 256), f32))
    good = jnp.max(jnp.where(most < HUGE, 0.0, 1.0)) == 0.0

    @pl.when(near & jnp.logical_not(good))
    def _():
        def again(t, carry):
            at = pl.multiple_of(t * 256, 256)
            state = one_row(all_rows(side_ref, ratio_ref, anchors_at(other_ref, start + at, 256)))
            at = pl.ds(at, 256)
            if stats:
                state = merged(known(at), state)
            store([(at, *state)])
            return carry

        lax.fori_loop(0, half // 256, again, 0)

    @pl.when(jnp.logical_not(near))
    def _():
        own = pl.ds(0, columns)
        for s in range(2):

            def exact(t, carry):
                at = pl.multiple_of(t * 256, 256)
                other = anchors_at(other_ref, start + at, 256)

                def block(b, state):
                    side_ref[own, :] = y_side(z_ref[b], emb)
                    v = score(side_ref[own, :], other)
                    if s:
                        v = v + wide(across(gap_of(z_ref[b], emb)), 256)
                    high = jnp.max(v, axis=0, keepdims=True)
                    return merged(state, (high, jnp.sum(jnp.exp2(v - high), axis=0, keepdims=True)))

                none = (jnp.full((1, 256), -1e30, jnp.float32), jnp.zeros((1, 256), jnp.float32))
                high, total = lax.fori_loop(0, blocks, block, none)
                lse_ref[s : s + 1, pl.ds(at, 256)] = high + jnp.log2(total)
                return carry

            lax.fori_loop(0, half // 256, exact, 0)


def column_sums(side, other_ref, start, lse_ref, tile, state_refs):
    columns = side.shape[0]
    piece = math.gcd(tile, PIECE)

    def some(at, v):
        lse = lse_ref[0:1, pl.ds(at, piece)]
        weight = jnp.exp2(jnp.clip(lse - lse_ref[1:2, pl.ds(at, piece)], -SPREAD, SPREAD))
        lse, weight = jnp.broadcast_to(lse, (8, piece)), jnp.broadcast_to(weight, (8, piece))
        parts = [slice(k, k + 128) for k in range(0, piece, 128)]
        for g in range(0, columns, 8):
            rows = slice(g, g + 8)
            u = [v[rows, p] - lse[:, p] for p in parts]
            top, sum0, sum1 = (ref[rows, :] for ref in state_refs)
            new = functools.reduce(jnp.maximum, u, top)
            less = jnp.exp2(top - new)
            e = [jnp.exp2(w - new) for w in u]
            state_refs[0][rows, :] = new
            state_refs[1][rows, :] = functools.reduce(jnp.add, e, sum0 * less)
            state_refs[2][rows, :] = functools.reduce(jnp.add, [w * weight[:, p] for w, p in zip(e, parts)], sum1 * less)

    def step(t, carry):
        ats = [pl.multiple_of(t * tile + k, piece) for k in range(0, tile, piece)]
        scores = [score(side, anchors_at(other_ref, start + at, piece)) for at in ats]
        for at, v in zip(ats, scores):
            some(at, v)
        return carry

    lax.fori_loop(0, lse_ref.shape[1] // tile, step, 0)


def columns_kernel(emb, tile, pairs, other_ref, z_ref, lse_ref, top_ref, sum0_ref, sum1_ref, side_ref):
    half = lse_ref.shape[1]
    side_ref[...] = y_side(z_ref[0], emb)
    top_ref[...] = jnp.full(top_ref.shape, -1e30, jnp.float32)
    sum0_ref[...] = jnp.zeros(sum0_ref.shape, jnp.float32)
    sum1_ref[...] = jnp.zeros(sum1_ref.shape, jnp.float32)
    column_sums(side_ref[...], other_ref, starting(pairs, half), lse_ref, tile, (top_ref, sum0_ref, sum1_ref))


def finish_kernel(emb, tile, pairs, shelters, other_ref, z_ref, *refs):
    lse_refs, refs = refs[:pairs], refs[pairs:]
    *old, anchor_hbm, column_ref, top_ref, sum0_ref, sum1_ref, side_ref, anchor_ref, sems = refs
    half = lse_refs[0].shape[1]
    mine = lax.rem(lax.axis_index("shel"), pairs)
    near = spread_of(z_ref, emb) <= SPREAD
    starts = [pl.multiple_of((mine ^ k) * half, half) for k in range(pairs)]
    side_ref[...] = y_side(z_ref[0], emb)
    states = (top_ref, sum0_ref, sum1_ref)
    writes = []
    for k, (start, lse_ref) in enumerate(zip(starts, lse_refs)):
        at = pl.ds(start, half)
        anchor_ref[:, at] = (-EPSILON * math.log(shelters)) - (EPSILON * math.log(2.0)) * lse_ref[...]
        writes.append(pltpu.make_async_copy(anchor_ref.at[:, at], anchor_hbm.at[:, at], sems.at[k]))
        writes[-1].start()
    for new, ref in zip(states, old):
        new[...] = ref[...]
    for start, lse_ref in list(zip(starts, lse_refs))[1:]:
        column_sums(side_ref[...], other_ref, start, lse_ref, tile, states)
    z = z_ref[0]
    h0, h1, f0, f1 = (z[emb + k : emb + k + 1] for k in range(4))
    offset = (-SCALE * f0 - math.log2(shelters), -SCALE * (h1 + f0 - h0) - math.log2(shelters))

    def one(top, *sums):
        top = top.T
        high = jnp.max(top, axis=0, keepdims=True)
        less = jnp.exp2(top - high)
        return [high + jnp.log2(jnp.sum(s.T * less, axis=0, keepdims=True)) for s in sums]

    for s, v in enumerate(one(*(ref[...] for ref in states))):
        column_ref[s : s + 1, :] = v + offset[s]

    @pl.when(jnp.logical_not(near))
    def _():
        for s in range(2):
            top_ref[...] = jnp.full(top_ref.shape, -1e30, jnp.float32)
            sum0_ref[...] = jnp.zeros(sum0_ref.shape, jnp.float32)
            for start, lse_ref in zip(starts, lse_refs):

                def column(t, carry):
                    at = pl.multiple_of(t * 256, 256)
                    other = anchors_at(other_ref, start + at, 256)
                    v = score(side_ref[...], other) - lse_ref[s : s + 1, pl.ds(at, 256)]
                    top = top_ref[...]
                    new = jnp.maximum(top, jnp.maximum(v[:, :128], v[:, 128:]))
                    sum0_ref[...] = sum0_ref[...] * jnp.exp2(top - new) + jnp.exp2(v[:, :128] - new) + jnp.exp2(v[:, 128:] - new)
                    top_ref[...] = new
                    return carry

                lax.fori_loop(0, half // 256, column, 0)
            column_ref[s : s + 1, :] = one(top_ref[...], sum0_ref[...])[0] + offset[s]

    for write in writes:
        write.wait()


def swapped(value, far, groups):
    return lax.ppermute(value, "shel", [(k, k ^ far) for k in range(groups)])


def on_device(anchor_embed, shelter_embed, hazard, shelter_pot):
    emb, rows = anchor_embed.shape
    columns = shelter_embed.shape[1]
    anchors = rows * lax.axis_size("orig")
    groups = lax.axis_size("shel")
    shelters = columns * groups
    pairs = 2 if groups % 2 == 0 else 1
    half = rows // pairs
    f32, bf16 = jnp.float32, jnp.bfloat16
    vmem = pl.BlockSpec(memory_space=pltpu.VMEM)

    def call(kernel, outs, ins, scratch, work, places=None):
        return pl.pallas_call(
            kernel,
            out_shape=outs,
            in_specs=[vmem] * len(ins),
            out_specs=places or jax.tree.map(lambda _: vmem, outs),
            scratch_shapes=scratch,
            compiler_params=pltpu.CompilerParams(vmem_limit_bytes=24 * 2**20),
            cost_estimate=pl.CostEstimate(flops=2 * DEPTH * work, bytes_accessed=DEPTH * rows, transcendentals=work),
        )(*ins)

    def sides(blocks):
        return [pltpu.VMEM((blocks * columns, DEPTH), bf16), pltpu.VMEM((blocks * columns, 128), f32)]

    shape = jax.ShapeDtypeStruct
    every = jnp.concatenate([shelter_embed, hazard, shelter_pot], axis=0)[None]
    other = call(
        functools.partial(anchors_kernel, math.gcd(rows, 1024)),
        shape((rows // 128, DEPTH, 128), bf16),
        [anchor_embed],
        [],
        64 * rows,
    )

    tile = math.gcd(half, 4096)

    def part(some):
        blocks = some.shape[0]
        return call(
            functools.partial(part_kernel, emb, tile, pairs),
            shape((8, half), f32),
            [other, some],
            sides(blocks),
            half * columns * blocks,
        )

    stats, done = [], 0
    if groups & (groups - 1) == 0:
        far = groups // 2
        while far:
            got = swapped(every, far, groups)
            if every.shape[0] > 1:
                stats.append(part(every[done:]))
                done = every.shape[0]
            every = jnp.concatenate([every, got], axis=0)
            far //= 2
    else:
        blocks = [lax.ppermute(every, "shel", [(k, (k + d) % groups) for k in range(groups)]) for d in range(1, groups)]
        every = jnp.concatenate([every, *blocks])
    lse = call(
        functools.partial(rest_kernel, emb, tile, pairs, done),
        shape((2, half), f32),
        [other, every, *stats],
        [*sides(groups - done), pltpu.VMEM((8 * (groups - done) + min(512, (groups - done) * columns), DEPTH), bf16)],
        half * columns * (groups - done),
    )

    tile = math.gcd(half, 4096)
    state = [shape((columns, 128), f32)] * 3
    lses = [lse] + ([swapped(lse, 1, groups)] if pairs == 2 else [])
    sums = call(
        functools.partial(columns_kernel, emb, tile, pairs),
        state,
        [other, every, lse],
        [pltpu.VMEM((columns, DEPTH), bf16)],
        half * columns,
    )
    anchor_pot, column = call(
        functools.partial(finish_kernel, emb, tile, pairs, shelters),
        (shape((2, rows), f32), shape((2, columns), f32)),
        [other, every, *lses, *sums],
        [pltpu.VMEM(s.shape, f32) for s in state]
        + [pltpu.VMEM((columns, DEPTH), bf16), pltpu.VMEM((2, rows), f32), pltpu.SemaphoreType.DMA((pairs,))],
        half * columns,
        (pl.BlockSpec(memory_space=pl.ANY), vmem),
    )

    halves = lax.axis_size("orig")
    parts = [column]
    for d in range(1, halves):
        parts.append(lax.ppermute(column, "orig", [(k, (k + d) % halves) for k in range(halves)]))
    high = functools.reduce(jnp.maximum, parts)
    total = sum(jnp.exp2(part - high) for part in parts)
    new_shelter_pot = -EPSILON * math.log(anchors) - (EPSILON * math.log(2.0)) * (high + jnp.log2(total))
    return anchor_pot, new_shelter_pot


def solution(mesh):
    placed = (
        P(None, ("region", "orig")),
        P(None, ("region", "shel")),
        P(None, ("region", "shel")),
        P(None, ("region", "shel")),
    )
    return jax.shard_map(
        on_device,
        mesh=mesh,
        in_specs=placed,
        out_specs=(P(None, ("region", "orig")), P(None, ("region", "shel"))),
        check_vma=False,
    )
```

```python
import functools
import math

import jax
import jax.numpy as jnp
from jax import lax
from jax.experimental import pallas as pl
from jax.experimental.pallas import tpu as pltpu
from jax.sharding import PartitionSpec as P

EPSILON = 0.25
SCALE = math.log2(math.e) / EPSILON
HUGE = 2.0**126
SPREAD = 36.0
PIECE = 512
DEPTH = 256


def three(v):
    a = v.astype(jnp.bfloat16).astype(jnp.float32)
    rest = v - a
    b = rest.astype(jnp.bfloat16).astype(jnp.float32)
    return a, b, (rest - b).astype(jnp.bfloat16).astype(jnp.float32)


def rows_of(values, count):
    width = next(v.shape[1] for v in values if not isinstance(v, float))
    index = lax.broadcasted_iota(jnp.int32, (count, width), 0)
    out = jnp.zeros((count, width), jnp.float32)
    for k, v in enumerate(values):
        out = jnp.where(index == k, v, out)
    return out


def x_side(x):
    emb = x.shape[0]
    x0, x1, x2 = three(x)
    norm = jnp.sum(x * x, axis=0, keepdims=True) * (-SCALE / emb)
    misc = rows_of((*three(norm), 1.0, 1.0, 1.0), DEPTH - 6 * emb)
    return jnp.concatenate([x0, x0, x1, x1, x0, x2, misc], axis=0).astype(jnp.bfloat16)


def gap_of(z, emb):
    h0, h1, f0, f1 = (z[emb + k : emb + k + 1] for k in range(4))
    return SCALE * ((f1 - h1) - (f0 - h0))


def y_side(z, emb):
    y = z[:emb]
    y0, y1, y2 = three(y * (2.0 * SCALE / emb))
    bias = SCALE * (z[emb + 2 : emb + 3] - z[emb : emb + 1]) - jnp.sum(y * y, axis=0, keepdims=True) * (SCALE / emb)
    misc = rows_of((1.0, 1.0, 1.0, *three(bias)), DEPTH - 6 * emb)
    side = jnp.concatenate([y0, y1, y0, y1, y2, y0, misc], axis=0)
    return side.T.astype(jnp.bfloat16)


def across(row):
    return jnp.broadcast_to(row, (128, row.shape[1])).T


def wide(block, width):
    return jnp.concatenate([block] * (width // 128), axis=1)


def score(side, other):
    return lax.dot_general(side, other, (((1,), (0,)), ((), ())), preferred_element_type=jnp.float32)


def row_sums(side, ratio, other):
    width = other.shape[1]
    count = side.shape[0]
    chunk = math.gcd(count, 128)
    v = score(side, other)
    state = None
    for c in range(0, count, chunk):
        part = v[c : c + chunk].reshape(chunk // 8, 8, width)
        r = wide(ratio[c : c + chunk], width).reshape(part.shape)
        new = jnp.max(part, axis=0)
        if state is not None:
            new = jnp.maximum(state[0], new)
        e = jnp.exp2(part - new)
        add0, add1 = jnp.sum(e, axis=0), jnp.sum(e * r, axis=0)
        if state is not None:
            less = jnp.exp2(state[0] - new)
            add0, add1 = state[1] * less + add0, state[2] * less + add1
        state = new, add0, add1
    return state


def merged(first, second):
    if first is None:
        return second
    high = jnp.maximum(first[0], second[0])
    one, two = jnp.exp2(first[0] - high), jnp.exp2(second[0] - high)
    return (high, *(a * one + b * two for a, b in zip(first[1:], second[1:])))


def one_row(state):
    top, sum0, sum1 = state
    high = jnp.max(top, axis=0, keepdims=True)
    less = jnp.exp2(top - high)
    return high, jnp.sum(sum0 * less, axis=0, keepdims=True), jnp.sum(sum1 * less, axis=0, keepdims=True)


def prepare(z, emb, side_ref, ratio_ref, slot):
    columns = z.shape[1]
    at = pl.ds(slot * columns, columns)
    side_ref[at, :] = y_side(z, emb)
    ratio_ref[at, :] = across(jnp.exp2(jnp.clip(gap_of(z, emb), -SPREAD, SPREAD)))


def all_rows(side_ref, ratio_ref, other):
    count = side_ref.shape[0]
    if count <= 512:
        return row_sums(side_ref[...], ratio_ref[...], other)

    def step(k, state):
        at = pl.ds(pl.multiple_of(k * 512, 512), 512)
        return merged(state, row_sums(side_ref[at, :], ratio_ref[at, :], other))

    return lax.fori_loop(1, count // 512, step, row_sums(side_ref[:512], ratio_ref[:512], other))


def anchors_at(other_ref, start, width):
    first = start // 128
    return jnp.concatenate([other_ref[first + k] for k in range(width // 128)], axis=1)


def starting(pairs, half):
    return pl.multiple_of(lax.rem(lax.axis_index("shel"), pairs) * half, half)


def anchors_kernel(tile, x_hbm, other_ref, x_ref, sems):
    def fetch(t):
        at = pl.ds(pl.multiple_of(t * tile, tile), tile)
        return pltpu.make_async_copy(x_hbm.at[:, at], x_ref.at[:, at], sems.at[t])

    def begin(t, carry):
        fetch(t).start()
        return carry

    lax.fori_loop(0, x_ref.shape[1] // tile, begin, 0)

    def step(t, carry):
        fetch(t).wait()
        side = x_side(x_ref[:, pl.ds(pl.multiple_of(t * tile, tile), tile)])
        for k in range(tile // 128):
            other_ref[t * (tile // 128) + k] = side[:, k * 128 : (k + 1) * 128]
        return carry

    lax.fori_loop(0, x_ref.shape[1] // tile, step, 0)


def part_kernel(emb, tile, pairs, other_ref, z_ref, stat_ref, side_ref, ratio_ref):
    half = stat_ref.shape[1]
    start = starting(pairs, half)
    for b in range(z_ref.shape[0]):
        prepare(z_ref[b], emb, side_ref, ratio_ref, b)

    def step(t, carry):
        found = []
        for part in range(0, tile, 256):
            at = pl.multiple_of(t * tile + part, 256)
            other = anchors_at(other_ref, start + at, 256)
            found.append((at, one_row(all_rows(side_ref, ratio_ref, other))))
        for at, state in found:
            for k, v in enumerate(state):
                stat_ref[k : k + 1, pl.ds(at, 256)] = v
        return carry

    lax.fori_loop(0, half // tile, step, 0)


def spread_of(z_ref, emb):
    z = z_ref[...]
    h0, h1, f0, f1 = (z[:, emb + k, :] for k in range(4))
    return jnp.max(jnp.abs(SCALE * ((f1 - h1) - (f0 - h0))))


def hottest(z, side, emb):
    columns = z.shape[1]
    value = jnp.broadcast_to(z[emb + 2 : emb + 3] - z[emb : emb + 1], (8, columns))
    row = lax.broadcasted_iota(jnp.int32, (8, columns), 0)
    lane = lax.broadcasted_iota(jnp.int32, (8, columns), 1)
    value = jnp.where(lax.rem(lane, 8) == row, value, -1e30)
    pick = (value == jnp.max(value, axis=1, keepdims=True)).astype(jnp.float32)
    pick = pick / jnp.sum(pick, axis=1, keepdims=True)
    return score(pick.astype(jnp.bfloat16), side).astype(jnp.bfloat16)


def rest_kernel(emb, tile, pairs, first, other_ref, z_ref, *refs):
    *stats, lse_ref, side_ref, ratio_ref, hot_ref = refs
    blocks, _, columns = z_ref.shape
    half = lse_ref.shape[1]
    start = starting(pairs, half)
    count = side_ref.shape[0]
    lead = hot_ref.shape[0] - min(count, 512)
    f32 = jnp.float32

    def ready(b):
        prepare(z_ref[b], emb, side_ref, ratio_ref, b - first)
        side = side_ref[pl.ds((b - first) * columns, columns), :]
        hot_ref[pl.ds((b - first) * 8, 8), :] = hottest(z_ref[b], side, emb)

    if blocks <= 8:
        for b in range(first, blocks):
            ready(b)
    else:
        lax.fori_loop(first, blocks, lambda b, c: (ready(b), c)[1], 0)
    hot_ref[lead:, :] = side_ref[: hot_ref.shape[0] - lead, :]
    near = spread_of(z_ref, emb) <= SPREAD

    def known(at):
        state = None
        for ref in stats:
            state = merged(state, tuple(ref[k : k + 1, at] for k in range(3)))
        return state

    def store(found):
        for at, high, *totals in found:
            for s in range(2):
                lse_ref[s : s + 1, at] = high + jnp.log2(totals[s])

    def sums(v, shift, ratio):
        e = jnp.exp2(v - shift)
        w = e * wide(ratio, 256)
        return [jnp.sum(u.reshape(u.shape[0] // 8, 8, 256), axis=0) for u in (e, w)]

    def step(t, most):
        found = []
        for part in range(0, tile, 256):
            at = pl.multiple_of(t * tile + part, 256)
            other = anchors_at(other_ref, start + at, 256)
            at = pl.ds(at, 256)
            state = known(at)
            v = score(hot_ref[...], other)
            shift = jnp.max(v[:lead], axis=0, keepdims=True)
            if state is not None:
                shift = jnp.maximum(shift, state[0])
            totals = sums(v[lead:], shift, ratio_ref[: count if count < 512 else 512, :])
            if count > 512:

                def more(k, totals):
                    at = pl.ds(pl.multiple_of(k * 512, 512), 512)
                    add = sums(score(side_ref[at, :], other), shift, ratio_ref[at, :])
                    return [a + b for a, b in zip(totals, add)]

                totals = lax.fori_loop(1, count // 512, more, totals)
            totals = [jnp.sum(u, axis=0, keepdims=True) for u in totals]
            if state is not None:
                less = jnp.exp2(state[0] - shift)
                totals = [u + w * less for u, w in zip(totals, state[1:])]
            most = jnp.maximum(most, jnp.maximum(*totals))
            found.append((at, shift, *totals))
        store(found)
        return most

    most = lax.fori_loop(0, half // tile, step, jnp.zeros((1, 256), f32))
    good = jnp.max(jnp.where(most < HUGE, 0.0, 1.0)) == 0.0

    @pl.when(near & jnp.logical_not(good))
    def _():
        def again(t, carry):
            at = pl.multiple_of(t * 256, 256)
            state = one_row(all_rows(side_ref, ratio_ref, anchors_at(other_ref, start + at, 256)))
            at = pl.ds(at, 256)
            if stats:
                state = merged(known(at), state)
            store([(at, *state)])
            return carry

        lax.fori_loop(0, half // 256, again, 0)

    @pl.when(jnp.logical_not(near))
    def _():
        own = pl.ds(0, columns)
        for s in range(2):

            def exact(t, carry):
                at = pl.multiple_of(t * 256, 256)
                other = anchors_at(other_ref, start + at, 256)

                def block(b, state):
                    side_ref[own, :] = y_side(z_ref[b], emb)
                    v = score(side_ref[own, :], other)
                    if s:
                        v = v + wide(across(gap_of(z_ref[b], emb)), 256)
                    high = jnp.max(v, axis=0, keepdims=True)
                    return merged(state, (high, jnp.sum(jnp.exp2(v - high), axis=0, keepdims=True)))

                none = (jnp.full((1, 256), -1e30, jnp.float32), jnp.zeros((1, 256), jnp.float32))
                high, total = lax.fori_loop(0, blocks, block, none)
                lse_ref[s : s + 1, pl.ds(at, 256)] = high + jnp.log2(total)
                return carry

            lax.fori_loop(0, half // 256, exact, 0)


def column_sums(scores_at, lse_ref, tile, state_refs):
    columns = state_refs[0].shape[0]
    piece = math.gcd(tile, PIECE)

    def some(at, v):
        lse = lse_ref[0:1, pl.ds(at, piece)]
        weight = jnp.exp2(jnp.clip(lse - lse_ref[1:2, pl.ds(at, piece)], -SPREAD, SPREAD))
        lse, weight = jnp.broadcast_to(lse, (8, piece)), jnp.broadcast_to(weight, (8, piece))
        parts = [slice(k, k + 128) for k in range(0, piece, 128)]
        for g in range(0, columns, 8):
            rows = slice(g, g + 8)
            u = [v[rows, p] - lse[:, p] for p in parts]
            top, sum0, sum1 = (ref[rows, :] for ref in state_refs)
            new = functools.reduce(jnp.maximum, u, top)
            less = jnp.exp2(top - new)
            e = [jnp.exp2(w - new) for w in u]
            state_refs[0][rows, :] = new
            state_refs[1][rows, :] = functools.reduce(jnp.add, e, sum0 * less)
            state_refs[2][rows, :] = functools.reduce(jnp.add, [w * weight[:, p] for w, p in zip(e, parts)], sum1 * less)

    def step(t, carry):
        ats = [pl.multiple_of(t * tile + k, piece) for k in range(0, tile, piece)]
        scores = [scores_at(at, piece) for at in ats]
        for at, v in zip(ats, scores):
            some(at, v)
        return carry

    lax.fori_loop(0, lse_ref.shape[1] // tile, step, 0)


def columns_kernel(emb, tile, pairs, other_ref, z_ref, lse_ref, top_ref, sum0_ref, sum1_ref, *refs):
    *later, side_ref = refs
    half = lse_ref.shape[1]
    start = starting(pairs, half)
    side_ref[...] = y_side(z_ref[0], emb)
    top_ref[...] = jnp.full(top_ref.shape, -1e30, jnp.float32)
    sum0_ref[...] = jnp.zeros(sum0_ref.shape, jnp.float32)
    sum1_ref[...] = jnp.zeros(sum1_ref.shape, jnp.float32)

    def scores_at(at, width):
        return score(side_ref[...], anchors_at(other_ref, start + at, width))

    column_sums(scores_at, lse_ref, tile, (top_ref, sum0_ref, sum1_ref))
    if later:

        def step(t, carry):
            for part in range(0, tile, 256):
                at = pl.multiple_of(t * tile + part, 256)
                later[0][:, pl.ds(at, 256)] = score(side_ref[...], anchors_at(other_ref, half - start + at, 256))
            return carry

        lax.fori_loop(0, half // tile, step, 0)


def finish_kernel(emb, tile, pairs, shelters, other_ref, z_ref, *refs):
    lse_refs, scores, refs = refs[:pairs], refs[pairs : 2 * pairs - 1], refs[2 * pairs - 1 :]
    *old, anchor_hbm, column_ref, top_ref, sum0_ref, sum1_ref, side_ref, anchor_ref, sems = refs
    half = lse_refs[0].shape[1]
    mine = lax.rem(lax.axis_index("shel"), pairs)
    near = spread_of(z_ref, emb) <= SPREAD
    starts = [pl.multiple_of((mine ^ k) * half, half) for k in range(pairs)]
    states = (top_ref, sum0_ref, sum1_ref)
    writes = []
    for k, (start, lse_ref) in enumerate(zip(starts, lse_refs)):
        at = pl.ds(start, half)
        anchor_ref[:, at] = (-EPSILON * math.log(shelters)) - (EPSILON * math.log(2.0)) * lse_ref[...]
        writes.append(pltpu.make_async_copy(anchor_ref.at[:, at], anchor_hbm.at[:, at], sems.at[k]))
        writes[-1].start()
    for new, ref in zip(states, old):
        new[...] = ref[...]
    for score_ref, lse_ref in zip(scores, lse_refs[1:]):
        column_sums(lambda at, width: score_ref[:, pl.ds(at, width)], lse_ref, tile, states)
    z = z_ref[0]
    h0, h1, f0, f1 = (z[emb + k : emb + k + 1] for k in range(4))
    offset = (-SCALE * f0 - math.log2(shelters), -SCALE * (h1 + f0 - h0) - math.log2(shelters))

    def one(top, *sums):
        top = top.T
        high = jnp.max(top, axis=0, keepdims=True)
        less = jnp.exp2(top - high)
        return [high + jnp.log2(jnp.sum(s.T * less, axis=0, keepdims=True)) for s in sums]

    for s, v in enumerate(one(*(ref[...] for ref in states))):
        column_ref[s : s + 1, :] = v + offset[s]

    @pl.when(jnp.logical_not(near))
    def _():
        side_ref[...] = y_side(z_ref[0], emb)
        for s in range(2):
            top_ref[...] = jnp.full(top_ref.shape, -1e30, jnp.float32)
            sum0_ref[...] = jnp.zeros(sum0_ref.shape, jnp.float32)
            for start, lse_ref in zip(starts, lse_refs):

                def column(t, carry):
                    at = pl.multiple_of(t * 256, 256)
                    other = anchors_at(other_ref, start + at, 256)
                    v = score(side_ref[...], other) - lse_ref[s : s + 1, pl.ds(at, 256)]
                    top = top_ref[...]
                    new = jnp.maximum(top, jnp.maximum(v[:, :128], v[:, 128:]))
                    sum0_ref[...] = sum0_ref[...] * jnp.exp2(top - new) + jnp.exp2(v[:, :128] - new) + jnp.exp2(v[:, 128:] - new)
                    top_ref[...] = new
                    return carry

                lax.fori_loop(0, half // 256, column, 0)
            column_ref[s : s + 1, :] = one(top_ref[...], sum0_ref[...])[0] + offset[s]

    for write in writes:
        write.wait()


def swapped(value, far, groups):
    return lax.ppermute(value, "shel", [(k, k ^ far) for k in range(groups)])


def on_device(anchor_embed, shelter_embed, hazard, shelter_pot):
    emb, rows = anchor_embed.shape
    columns = shelter_embed.shape[1]
    anchors = rows * lax.axis_size("orig")
    groups = lax.axis_size("shel")
    shelters = columns * groups
    pairs = 2 if groups % 2 == 0 else 1
    half = rows // pairs
    f32, bf16 = jnp.float32, jnp.bfloat16
    vmem = pl.BlockSpec(memory_space=pltpu.VMEM)

    def call(kernel, outs, ins, scratch, work, places=None, first=None):
        return pl.pallas_call(
            kernel,
            out_shape=outs,
            in_specs=[first or vmem] + [vmem] * (len(ins) - 1),
            out_specs=places or jax.tree.map(lambda _: vmem, outs),
            scratch_shapes=scratch,
            compiler_params=pltpu.CompilerParams(vmem_limit_bytes=24 * 2**20),
            cost_estimate=pl.CostEstimate(flops=2 * DEPTH * work, bytes_accessed=DEPTH * rows, transcendentals=work),
        )(*ins)

    def sides(blocks):
        return [pltpu.VMEM((blocks * columns, DEPTH), bf16), pltpu.VMEM((blocks * columns, 128), f32)]

    shape = jax.ShapeDtypeStruct
    every = jnp.concatenate([shelter_embed, hazard, shelter_pot], axis=0)[None]
    other = call(
        functools.partial(anchors_kernel, math.gcd(rows, 1024)),
        shape((rows // 128, DEPTH, 128), bf16),
        [pltpu.with_memory_space_constraint(anchor_embed, pltpu.HBM)],
        [pltpu.VMEM((emb, rows), f32), pltpu.SemaphoreType.DMA((rows // math.gcd(rows, 1024),))],
        64 * rows,
        first=pl.BlockSpec(memory_space=pltpu.HBM),
    )

    tile = math.gcd(half, 4096)

    def part(some):
        blocks = some.shape[0]
        return call(
            functools.partial(part_kernel, emb, tile, pairs),
            shape((8, half), f32),
            [other, some],
            sides(blocks),
            half * columns * blocks,
        )

    stats, done = [], 0
    if groups & (groups - 1) == 0:
        far = groups // 2
        while far:
            got = swapped(every, far, groups)
            if every.shape[0] > 1:
                stats.append(part(every[done:]))
                done = every.shape[0]
            every = jnp.concatenate([every, got], axis=0)
            far //= 2
    else:
        blocks = [lax.ppermute(every, "shel", [(k, (k + d) % groups) for k in range(groups)]) for d in range(1, groups)]
        every = jnp.concatenate([every, *blocks])
    lse = call(
        functools.partial(rest_kernel, emb, tile, pairs, done),
        shape((2, half), f32),
        [other, every, *stats],
        [*sides(groups - done), pltpu.VMEM((8 * (groups - done) + min(512, (groups - done) * columns), DEPTH), bf16)],
        half * columns * (groups - done),
    )

    tile = math.gcd(half, 4096)
    state = [shape((columns, 128), f32)] * 3
    lses = [lse] + ([swapped(lse, 1, groups)] if pairs == 2 else [])
    later = [shape((columns, half), f32)] * (pairs - 1)
    found = call(
        functools.partial(columns_kernel, emb, tile, pairs),
        state + later,
        [other, every, lse],
        [pltpu.VMEM((columns, DEPTH), bf16)],
        half * columns * pairs,
    )
    sums, scores = found[:3], found[3:]
    anchor_pot, column = call(
        functools.partial(finish_kernel, emb, tile, pairs, shelters),
        (shape((2, rows), f32), shape((2, columns), f32)),
        [other, every, *lses, *scores, *sums],
        [pltpu.VMEM(s.shape, f32) for s in state]
        + [pltpu.VMEM((columns, DEPTH), bf16), pltpu.VMEM((2, rows), f32), pltpu.SemaphoreType.DMA((pairs,))],
        half * columns,
        (pl.BlockSpec(memory_space=pl.ANY), vmem),
    )

    halves = lax.axis_size("orig")
    parts = [column]
    for d in range(1, halves):
        parts.append(lax.ppermute(column, "orig", [(k, (k + d) % halves) for k in range(halves)]))
    high = functools.reduce(jnp.maximum, parts)
    total = sum(jnp.exp2(part - high) for part in parts)
    new_shelter_pot = -EPSILON * math.log(anchors) - (EPSILON * math.log(2.0)) * (high + jnp.log2(total))
    return anchor_pot, new_shelter_pot


def solution(mesh):
    placed = (
        P(None, ("region", "orig")),
        P(None, ("region", "shel")),
        P(None, ("region", "shel")),
        P(None, ("region", "shel")),
    )
    return jax.shard_map(
        on_device,
        mesh=mesh,
        in_specs=placed,
        out_specs=(P(None, ("region", "orig")), P(None, ("region", "shel"))),
        check_vma=False,
    )
```

```python
import functools
import math

import jax
import jax.numpy as jnp
from jax import lax
from jax.experimental import pallas as pl
from jax.experimental.pallas import tpu as pltpu
from jax.sharding import PartitionSpec as P

EPSILON = 0.25
SCALE = math.log2(math.e) / EPSILON
HUGE = 2.0**126
SPREAD = 36.0
PIECE = 512
DEPTH = 256


def three(v):
    a = v.astype(jnp.bfloat16).astype(jnp.float32)
    rest = v - a
    b = rest.astype(jnp.bfloat16).astype(jnp.float32)
    return a, b, (rest - b).astype(jnp.bfloat16).astype(jnp.float32)


def rows_of(values, count):
    width = next(v.shape[1] for v in values if not isinstance(v, float))
    index = lax.broadcasted_iota(jnp.int32, (count, width), 0)
    out = jnp.zeros((count, width), jnp.float32)
    for k, v in enumerate(values):
        out = jnp.where(index == k, v, out)
    return out


def x_side(x):
    emb = x.shape[0]
    x0, x1, x2 = three(x)
    norm = jnp.sum(x * x, axis=0, keepdims=True) * (-SCALE / emb)
    misc = rows_of((*three(norm), 1.0, 1.0, 1.0), DEPTH - 6 * emb)
    return jnp.concatenate([x0, x0, x1, x1, x0, x2, misc], axis=0).astype(jnp.bfloat16)


def gap_of(z, emb):
    h0, h1, f0, f1 = (z[emb + k : emb + k + 1] for k in range(4))
    return SCALE * ((f1 - h1) - (f0 - h0))


def y_side(z, emb):
    y = z[:emb]
    y0, y1, y2 = three(y * (2.0 * SCALE / emb))
    bias = SCALE * (z[emb + 2 : emb + 3] - z[emb : emb + 1]) - jnp.sum(y * y, axis=0, keepdims=True) * (SCALE / emb)
    misc = rows_of((1.0, 1.0, 1.0, *three(bias)), DEPTH - 6 * emb)
    side = jnp.concatenate([y0, y1, y0, y1, y2, y0, misc], axis=0)
    return side.T.astype(jnp.bfloat16)


def across(row):
    return jnp.broadcast_to(row, (128, row.shape[1])).T


def wide(block, width):
    return jnp.concatenate([block] * (width // 128), axis=1)


def score(side, other):
    return lax.dot_general(side, other, (((1,), (0,)), ((), ())), preferred_element_type=jnp.float32)


def row_sums(side, ratio, other):
    width = other.shape[1]
    count = side.shape[0]
    chunk = math.gcd(count, 128)
    v = score(side, other)
    state = None
    for c in range(0, count, chunk):
        part = v[c : c + chunk].reshape(chunk // 8, 8, width)
        r = wide(ratio[c : c + chunk], width).reshape(part.shape)
        new = jnp.max(part, axis=0)
        if state is not None:
            new = jnp.maximum(state[0], new)
        e = jnp.exp2(part - new)
        add0, add1 = jnp.sum(e, axis=0), jnp.sum(e * r, axis=0)
        if state is not None:
            less = jnp.exp2(state[0] - new)
            add0, add1 = state[1] * less + add0, state[2] * less + add1
        state = new, add0, add1
    return state


def merged(first, second):
    if first is None:
        return second
    high = jnp.maximum(first[0], second[0])
    one, two = jnp.exp2(first[0] - high), jnp.exp2(second[0] - high)
    return (high, *(a * one + b * two for a, b in zip(first[1:], second[1:])))


def one_row(state):
    top, sum0, sum1 = state
    high = jnp.max(top, axis=0, keepdims=True)
    less = jnp.exp2(top - high)
    return high, jnp.sum(sum0 * less, axis=0, keepdims=True), jnp.sum(sum1 * less, axis=0, keepdims=True)


def prepare(z, emb, side_ref, ratio_ref, slot):
    columns = z.shape[1]
    at = pl.ds(slot * columns, columns)
    side_ref[at, :] = y_side(z, emb)
    ratio_ref[at, :] = across(jnp.exp2(jnp.clip(gap_of(z, emb), -SPREAD, SPREAD)))


def all_rows(side_ref, ratio_ref, other):
    count = side_ref.shape[0]
    if count <= 512:
        return row_sums(side_ref[...], ratio_ref[...], other)

    def step(k, state):
        at = pl.ds(pl.multiple_of(k * 512, 512), 512)
        return merged(state, row_sums(side_ref[at, :], ratio_ref[at, :], other))

    return lax.fori_loop(1, count // 512, step, row_sums(side_ref[:512], ratio_ref[:512], other))


def anchors_at(other_ref, start, width):
    first = start // 128
    return jnp.concatenate([other_ref[first + k] for k in range(width // 128)], axis=1)


def starting(pairs, half):
    return pl.multiple_of(lax.rem(lax.axis_index("shel"), pairs) * half, half)


def anchors_kernel(tile, x_hbm, other_ref, x_ref, sems):
    def fetch(t):
        at = pl.ds(pl.multiple_of(t * tile, tile), tile)
        return pltpu.make_async_copy(x_hbm.at[:, at], x_ref.at[:, at], sems.at[t])

    def begin(t, carry):
        fetch(t).start()
        return carry

    lax.fori_loop(0, x_ref.shape[1] // tile, begin, 0)

    def step(t, carry):
        fetch(t).wait()
        side = x_side(x_ref[:, pl.ds(pl.multiple_of(t * tile, tile), tile)])
        for k in range(tile // 128):
            other_ref[t * (tile // 128) + k] = side[:, k * 128 : (k + 1) * 128]
        return carry

    lax.fori_loop(0, x_ref.shape[1] // tile, step, 0)


def part_kernel(emb, tile, pairs, other_ref, z_ref, stat_ref, side_ref, ratio_ref):
    half = stat_ref.shape[1]
    start = starting(pairs, half)
    for b in range(z_ref.shape[0]):
        prepare(z_ref[b], emb, side_ref, ratio_ref, b)

    def step(t, carry):
        found = []
        for part in range(0, tile, 256):
            at = pl.multiple_of(t * tile + part, 256)
            other = anchors_at(other_ref, start + at, 256)
            found.append((at, one_row(all_rows(side_ref, ratio_ref, other))))
        for at, state in found:
            for k, v in enumerate(state):
                stat_ref[k : k + 1, pl.ds(at, 256)] = v
        return carry

    lax.fori_loop(0, half // tile, step, 0)


def spread_of(z_ref, emb):
    z = z_ref[...]
    h0, h1, f0, f1 = (z[:, emb + k, :] for k in range(4))
    return jnp.max(jnp.abs(SCALE * ((f1 - h1) - (f0 - h0))))


def hottest(z, side, emb):
    columns = z.shape[1]
    value = jnp.broadcast_to(z[emb + 2 : emb + 3] - z[emb : emb + 1], (8, columns))
    row = lax.broadcasted_iota(jnp.int32, (8, columns), 0)
    lane = lax.broadcasted_iota(jnp.int32, (8, columns), 1)
    value = jnp.where(lax.rem(lane, 8) == row, value, -1e30)
    pick = (value == jnp.max(value, axis=1, keepdims=True)).astype(jnp.float32)
    pick = pick / jnp.sum(pick, axis=1, keepdims=True)
    return score(pick.astype(jnp.bfloat16), side).astype(jnp.bfloat16)


def rest_kernel(emb, tile, pairs, first, other_ref, z_ref, *refs):
    *stats, lse_ref, side_ref, ratio_ref, hot_ref = refs
    blocks, _, columns = z_ref.shape
    half = lse_ref.shape[1]
    start = starting(pairs, half)
    count = side_ref.shape[0]
    lead = hot_ref.shape[0] - min(count, 512)
    f32 = jnp.float32

    def ready(b):
        prepare(z_ref[b], emb, side_ref, ratio_ref, b - first)
        side = side_ref[pl.ds((b - first) * columns, columns), :]
        hot_ref[pl.ds((b - first) * 8, 8), :] = hottest(z_ref[b], side, emb)

    if blocks <= 8:
        for b in range(first, blocks):
            ready(b)
    else:
        lax.fori_loop(first, blocks, lambda b, c: (ready(b), c)[1], 0)
    hot_ref[lead:, :] = side_ref[: hot_ref.shape[0] - lead, :]
    near = spread_of(z_ref, emb) <= SPREAD

    def known(at):
        state = None
        for ref in stats:
            state = merged(state, tuple(ref[k : k + 1, at] for k in range(3)))
        return state

    def store(found):
        for at, high, *totals in found:
            for s in range(2):
                lse_ref[s : s + 1, at] = high + jnp.log2(totals[s])

    def sums(v, shift, ratio):
        e = jnp.exp2(v - shift)
        w = e * wide(ratio, 256)
        return [jnp.sum(u.reshape(u.shape[0] // 8, 8, 256), axis=0) for u in (e, w)]

    def step(t, most):
        found = []
        for part in range(0, tile, 256):
            at = pl.multiple_of(t * tile + part, 256)
            other = anchors_at(other_ref, start + at, 256)
            at = pl.ds(at, 256)
            state = known(at)
            v = score(hot_ref[...], other)
            shift = jnp.max(v[:lead], axis=0, keepdims=True)
            if state is not None:
                shift = jnp.maximum(shift, state[0])
            totals = sums(v[lead:], shift, ratio_ref[: count if count < 512 else 512, :])
            if count > 512:

                def more(k, totals):
                    at = pl.ds(pl.multiple_of(k * 512, 512), 512)
                    add = sums(score(side_ref[at, :], other), shift, ratio_ref[at, :])
                    return [a + b for a, b in zip(totals, add)]

                totals = lax.fori_loop(1, count // 512, more, totals)
            totals = [jnp.sum(u, axis=0, keepdims=True) for u in totals]
            if state is not None:
                less = jnp.exp2(state[0] - shift)
                totals = [u + w * less for u, w in zip(totals, state[1:])]
            most = jnp.maximum(most, jnp.maximum(*totals))
            found.append((at, shift, *totals))
        store(found)
        return most

    most = lax.fori_loop(0, half // tile, step, jnp.zeros((1, 256), f32))
    good = jnp.max(jnp.where(most < HUGE, 0.0, 1.0)) == 0.0

    @pl.when(near & jnp.logical_not(good))
    def _():
        def again(t, carry):
            at = pl.multiple_of(t * 256, 256)
            state = one_row(all_rows(side_ref, ratio_ref, anchors_at(other_ref, start + at, 256)))
            at = pl.ds(at, 256)
            if stats:
                state = merged(known(at), state)
            store([(at, *state)])
            return carry

        lax.fori_loop(0, half // 256, again, 0)

    @pl.when(jnp.logical_not(near))
    def _():
        own = pl.ds(0, columns)
        for s in range(2):

            def exact(t, carry):
                at = pl.multiple_of(t * 256, 256)
                other = anchors_at(other_ref, start + at, 256)

                def block(b, state):
                    side_ref[own, :] = y_side(z_ref[b], emb)
                    v = score(side_ref[own, :], other)
                    if s:
                        v = v + wide(across(gap_of(z_ref[b], emb)), 256)
                    high = jnp.max(v, axis=0, keepdims=True)
                    return merged(state, (high, jnp.sum(jnp.exp2(v - high), axis=0, keepdims=True)))

                none = (jnp.full((1, 256), -1e30, jnp.float32), jnp.zeros((1, 256), jnp.float32))
                high, total = lax.fori_loop(0, blocks, block, none)
                lse_ref[s : s + 1, pl.ds(at, 256)] = high + jnp.log2(total)
                return carry

            lax.fori_loop(0, half // 256, exact, 0)


def column_sums(scores_at, lse_ref, tile, state_refs):
    columns = state_refs[0].shape[0]
    piece = math.gcd(tile, PIECE)

    def some(at, v):
        lse = lse_ref[0:1, pl.ds(at, piece)]
        weight = jnp.exp2(jnp.clip(lse - lse_ref[1:2, pl.ds(at, piece)], -SPREAD, SPREAD))
        lse, weight = jnp.broadcast_to(lse, (8, piece)), jnp.broadcast_to(weight, (8, piece))
        parts = [slice(k, k + 128) for k in range(0, piece, 128)]
        for g in range(0, columns, 8):
            rows = slice(g, g + 8)
            u = [v[rows, p] - lse[:, p] for p in parts]
            top, sum0, sum1 = (ref[rows, :] for ref in state_refs)
            new = functools.reduce(jnp.maximum, u, top)
            less = jnp.exp2(top - new)
            e = [jnp.exp2(w - new) for w in u]
            state_refs[0][rows, :] = new
            state_refs[1][rows, :] = functools.reduce(jnp.add, e, sum0 * less)
            state_refs[2][rows, :] = functools.reduce(jnp.add, [w * weight[:, p] for w, p in zip(e, parts)], sum1 * less)

    def step(t, carry):
        ats = [pl.multiple_of(t * tile + k, piece) for k in range(0, tile, piece)]
        scores = [scores_at(at, piece) for at in ats]
        for at, v in zip(ats, scores):
            some(at, v)
        return carry

    lax.fori_loop(0, lse_ref.shape[1] // tile, step, 0)


def columns_kernel(emb, tile, pairs, other_ref, z_ref, lse_ref, top_ref, sum0_ref, sum1_ref, *refs):
    *later, side_ref = refs
    half = lse_ref.shape[1]
    start = starting(pairs, half)
    side_ref[...] = y_side(z_ref[0], emb)
    top_ref[...] = jnp.full(top_ref.shape, -1e30, jnp.float32)
    sum0_ref[...] = jnp.zeros(sum0_ref.shape, jnp.float32)
    sum1_ref[...] = jnp.zeros(sum1_ref.shape, jnp.float32)

    def scores_at(at, width):
        return score(side_ref[...], anchors_at(other_ref, start + at, width))

    column_sums(scores_at, lse_ref, tile, (top_ref, sum0_ref, sum1_ref))
    if later:

        def step(t, carry):
            for part in range(0, tile, 256):
                at = pl.multiple_of(t * tile + part, 256)
                later[0][:, pl.ds(at, 256)] = score(side_ref[...], anchors_at(other_ref, half - start + at, 256))
            return carry

        lax.fori_loop(0, half // tile, step, 0)


def finish_kernel(emb, tile, pairs, shelters, other_ref, z_ref, *refs):
    lse_refs, scores, refs = refs[:pairs], refs[pairs : 2 * pairs - 1], refs[2 * pairs - 1 :]
    *old, anchor_hbm, column_ref, top_ref, sum0_ref, sum1_ref, side_ref, anchor_ref, sems = refs
    half = lse_refs[0].shape[1]
    mine = lax.rem(lax.axis_index("shel"), pairs)
    near = spread_of(z_ref, emb) <= SPREAD
    starts = [pl.multiple_of((mine ^ k) * half, half) for k in range(pairs)]
    states = (top_ref, sum0_ref, sum1_ref)
    writes = []
    for k, (start, lse_ref) in enumerate(zip(starts, lse_refs)):
        at = pl.ds(start, half)
        anchor_ref[:, at] = (-EPSILON * math.log(shelters)) - (EPSILON * math.log(2.0)) * lse_ref[...]
        writes.append(pltpu.make_async_copy(anchor_ref.at[:, at], anchor_hbm.at[:, at], sems.at[k]))
        writes[-1].start()
    for new, ref in zip(states, old):
        new[...] = ref[...]
    for score_ref, lse_ref in zip(scores, lse_refs[1:]):
        column_sums(lambda at, width: score_ref[:, pl.ds(at, width)], lse_ref, tile, states)
    z = z_ref[0]
    h0, h1, f0, f1 = (z[emb + k : emb + k + 1] for k in range(4))
    offset = (-SCALE * f0 - math.log2(shelters), -SCALE * (h1 + f0 - h0) - math.log2(shelters))

    def one(top, *sums):
        top = top.T
        high = jnp.max(top, axis=0, keepdims=True)
        less = jnp.exp2(top - high)
        return [high + jnp.log2(jnp.sum(s.T * less, axis=0, keepdims=True)) for s in sums]

    for s, v in enumerate(one(*(ref[...] for ref in states))):
        column_ref[s : s + 1, :] = v + offset[s]

    @pl.when(jnp.logical_not(near))
    def _():
        side_ref[...] = y_side(z_ref[0], emb)
        for s in range(2):
            top_ref[...] = jnp.full(top_ref.shape, -1e30, jnp.float32)
            sum0_ref[...] = jnp.zeros(sum0_ref.shape, jnp.float32)
            for start, lse_ref in zip(starts, lse_refs):

                def column(t, carry):
                    at = pl.multiple_of(t * 256, 256)
                    other = anchors_at(other_ref, start + at, 256)
                    v = score(side_ref[...], other) - lse_ref[s : s + 1, pl.ds(at, 256)]
                    top = top_ref[...]
                    new = jnp.maximum(top, jnp.maximum(v[:, :128], v[:, 128:]))
                    sum0_ref[...] = sum0_ref[...] * jnp.exp2(top - new) + jnp.exp2(v[:, :128] - new) + jnp.exp2(v[:, 128:] - new)
                    top_ref[...] = new
                    return carry

                lax.fori_loop(0, half // 256, column, 0)
            column_ref[s : s + 1, :] = one(top_ref[...], sum0_ref[...])[0] + offset[s]

    for write in writes:
        write.wait()


def swapped(value, far, groups):
    return lax.ppermute(value, "shel", [(k, k ^ far) for k in range(groups)])


def on_device(anchor_embed, shelter_embed, hazard, shelter_pot):
    emb, rows = anchor_embed.shape
    columns = shelter_embed.shape[1]
    anchors = rows * lax.axis_size("orig")
    groups = lax.axis_size("shel")
    shelters = columns * groups
    pairs = 2 if groups % 2 == 0 else 1
    half = rows // pairs
    f32, bf16 = jnp.float32, jnp.bfloat16
    vmem = pl.BlockSpec(memory_space=pltpu.VMEM)

    def call(kernel, outs, ins, scratch, work, places=None, first=None, flags=None):
        return pl.pallas_call(
            kernel,
            out_shape=outs,
            in_specs=[first or vmem] + [vmem] * (len(ins) - 1),
            out_specs=places or jax.tree.map(lambda _: vmem, outs),
            scratch_shapes=scratch,
            compiler_params=pltpu.CompilerParams(vmem_limit_bytes=24 * 2**20, flags=flags),
            cost_estimate=pl.CostEstimate(flops=2 * DEPTH * work, bytes_accessed=DEPTH * rows, transcendentals=work),
        )(*ins)

    def sides(blocks):
        return [pltpu.VMEM((blocks * columns, DEPTH), bf16), pltpu.VMEM((blocks * columns, 128), f32)]

    shape = jax.ShapeDtypeStruct
    every = jnp.concatenate([shelter_embed, hazard, shelter_pot], axis=0)[None]
    other = call(
        functools.partial(anchors_kernel, math.gcd(rows, 1024)),
        shape((rows // 128, DEPTH, 128), bf16),
        [pltpu.with_memory_space_constraint(anchor_embed, pltpu.HBM)],
        [pltpu.VMEM((emb, rows), f32), pltpu.SemaphoreType.DMA((rows // math.gcd(rows, 1024),))],
        64 * rows,
        first=pl.BlockSpec(memory_space=pltpu.HBM),
    )

    tile = math.gcd(half, 4096)

    def part(some):
        blocks = some.shape[0]
        return call(
            functools.partial(part_kernel, emb, tile, pairs),
            shape((8, half), f32),
            [other, some],
            sides(blocks),
            half * columns * blocks,
        )

    stats, done = [], 0
    if groups & (groups - 1) == 0:
        far = groups // 2
        while far:
            got = swapped(every, far, groups)
            if every.shape[0] > 1:
                stats.append(part(every[done:]))
                done = every.shape[0]
            every = jnp.concatenate([every, got], axis=0)
            far //= 2
    else:
        blocks = [lax.ppermute(every, "shel", [(k, (k + d) % groups) for k in range(groups)]) for d in range(1, groups)]
        every = jnp.concatenate([every, *blocks])
    lse = call(
        functools.partial(rest_kernel, emb, tile, pairs, done),
        shape((2, half), f32),
        [other, every, *stats],
        [*sides(groups - done), pltpu.VMEM((8 * (groups - done) + min(512, (groups - done) * columns), DEPTH), bf16)],
        half * columns * (groups - done),
    )

    tile = math.gcd(half, 4096)
    state = [shape((columns, 128), f32)] * 3
    lses = [lse] + ([swapped(lse, 1, groups)] if pairs == 2 else [])
    later = [shape((columns, half), f32)] * (pairs - 1)
    found = call(
        functools.partial(columns_kernel, emb, tile, pairs),
        state + later,
        [other, every, lse],
        [pltpu.VMEM((columns, DEPTH), bf16)],
        half * columns * pairs,
    )
    sums, scores = found[:3], found[3:]
    anchor_pot, column = call(
        functools.partial(finish_kernel, emb, tile, pairs, shelters),
        (shape((2, rows), f32), shape((2, columns), f32)),
        [other, every, *lses, *scores, *sums],
        [pltpu.VMEM(s.shape, f32) for s in state]
        + [pltpu.VMEM((columns, DEPTH), bf16), pltpu.VMEM((2, rows), f32), pltpu.SemaphoreType.DMA((pairs,))],
        half * columns,
        (pl.BlockSpec(memory_space=pl.ANY), vmem),
    )

    halves = lax.axis_size("orig")
    parts = [column]
    for d in range(1, halves):
        parts.append(lax.ppermute(column, "orig", [(k, (k + d) % halves) for k in range(halves)]))
    high = functools.reduce(jnp.maximum, parts)
    total = sum(jnp.exp2(part - high) for part in parts)
    new_shelter_pot = -EPSILON * math.log(anchors) - (EPSILON * math.log(2.0)) * (high + jnp.log2(total))
    return anchor_pot, new_shelter_pot


def solution(mesh):
    placed = (
        P(None, ("region", "orig")),
        P(None, ("region", "shel")),
        P(None, ("region", "shel")),
        P(None, ("region", "shel")),
    )
    return jax.shard_map(
        on_device,
        mesh=mesh,
        in_specs=placed,
        out_specs=(P(None, ("region", "orig")), P(None, ("region", "shel"))),
        check_vma=False,
    )
```
